128 devices in a mesh: row: 16 (over x, y_lo, core), col: 8 (over y_hi, z).
Axes of the slice: x: 4, y: 4 (y_hi: 2, y_lo: 2; y = y_hi * 2 + y_lo), z: 4, core: 2. Of those that a mesh axis runs over, the one named last changes fastest.
Arguments:
- pair_in: bfloat16 [768, 768, 128], P('row', 'col'), may hold values from -6 to 6
- coords: float32 [3, 768], P(None, 'row'), may hold values from -36 to 36
- chain_ids: int32 [768], P('row'), may hold values from 0 to 3, never falling along the last dimension, each value on 1 to 384 neighbouring positions
- coord_mask: int32 [768], P('row'), may hold values 0 or 1
- gain_tri: float32 [128], replicated, may hold values from 0.1 to 1.9
- gain_sum: float32 [128], replicated, may hold values from 0.1 to 1.9
- gain_attn: float32 [128], replicated, may hold values from 0.1 to 1.9
- w_tri_in: bfloat16 [128, 640], replicated, may hold values from -0.5 to 0.5
- w_tri_out: bfloat16 [128, 128], replicated, may hold values from -0.5 to 0.5
- w_bins: float32 [36, 128], replicated, may hold values from -3 to 3
- same_chain: float32 [128], replicated, may hold values from -6 to 6
- w_query: bfloat16 [128, 128], replicated, may hold values from -8 to 8
- w_attn: bfloat16 [128, 384], replicated, may hold values from -0.5 to 0.5
- w_bias: bfloat16 [128, 4], replicated, may hold values from -0.5 to 0.5
- w_attn_out: bfloat16 [128, 128], replicated, may hold values from -0.5 to 0.5
Outputs:
- pair_out: bfloat16 [768, 768, 128], P('row', 'col')
The draws below stay inside these ranges and needn't reach their ends.
Inputs may be any that keep to these rules, and one draw needn't show every extreme that they name: `chain_ids`: chain numbers never fall along the residues, and no chain holds more than half of them.
All inputs are finite; a program needn't handle non-finite values. No bound on the sum of `coord_mask` on one device may be relied on, other than what follows from the above.
Results may differ from the reference program's by a relative error of at most 0.02.
Values may be sent and summed in bfloat16 or wider, within the bound.
No kernel may reach another device: no remote copies, remote signals or barrier semaphores. Data moves between devices by JAX's collectives and lax.ppermute only.
A program may use at most 192 MiB of HBM per device.

```python
import math
import jax
import jax.numpy as jnp
import numpy as np
from jax import lax

CP = 128
HEADS = 4
HEAD_DIM = 32
NBINS = 36
L = 768


def draw_w_query(key, part):
    first_key = jax.random.fold_in(key, 11)
    second_key = jax.random.fold_in(key, 12)
    base = jnp.clip(jax.random.normal(first_key, (CP, CP), jnp.float32), -4.0, 4.0) * CP ** (-0.5)
    factor = jnp.exp(jax.random.uniform(second_key, (HEADS,), jnp.float32, jnp.log(0.5), jnp.log(2.0)))
    scaled = base * jnp.repeat(factor, CP // HEADS)[None, :]
    return jnp.clip(scaled, -8.0, 8.0).astype(jnp.bfloat16)


def with_ends(values, rng, least, top_value):
    shape = values.shape
    index_at = [jax.random.randint(jax.random.fold_in(rng, axis), (), 0, shape[axis]) for axis in range(len(shape))]
    values = values.at[tuple(index_at)].set(least)
    longest = shape.index(max(shape))
    index_at[longest] = (index_at[longest] + 1) % shape[longest]
    return values.at[tuple(index_at)].set(top_value)


def block_scale(rng, shape, pieces, smallest, largest):
    def one(axis_at, parts):
        steps = jax.random.uniform(jax.random.fold_in(jax.random.fold_in(rng, 6), axis_at), (parts,), jnp.float32, smallest / len(pieces), largest / len(pieces))
        return jnp.repeat(jnp.exp(steps), shape[axis_at] // parts).reshape((-1,) + (1,) * (len(shape) - axis_at - 1))

    loudness = one(*pieces[0])
    for cut in pieces[1:]:
        loudness = loudness * one(*cut)
    return loudness


def profile(count, total, reach, lean):
    loads = [(1 << 20) // math.isqrt(standing ** lean) + 1 for standing in range(2, count + 1)]
    spare, holding = total - reach - (count - 1), [1] * (count - 1)
    while spare > 0:
        movable = [i for i in range(count - 1) if holding[i] < reach]
        pool, remaining = sum([loads[i] for i in movable]), spare
        for i in movable:
            extra = min(reach - holding[i], max(1, remaining * loads[i] // pool), spare)
            holding[i] = holding[i] + extra
            spare = spare - extra
    return np.array([reach] + holding)


def ragged(key, count, total, limit, skew):
    if count == 2:
        one = jax.random.randint(key, (), max(1, total - limit), min(limit, total - 1) + 1)
        return jnp.stack([one, total - one])
    lengths = jnp.asarray(profile(count, total, limit, skew), jnp.int32)
    pairs = (count - 1) // 2
    donor, receiver = lengths[1:1 + 2 * pairs:2], lengths[2:2 + 2 * pairs:2]
    room = jnp.minimum(donor - 1, limit - receiver)
    moved = jax.random.randint(jax.random.fold_in(key, 1), (pairs,), 0, 1 << 20) % (room + 1)
    lengths = lengths.at[1:1 + 2 * pairs:2].set(donor - moved).at[2:2 + 2 * pairs:2].set(receiver + moved)
    return lengths[jax.random.permutation(jax.random.fold_in(key, 2), count)]


def scatter_about(stream_key, shape, scale, most, shards=(), kind=jnp.bfloat16):
    level = block_scale(stream_key, shape, shards, -0.22, 0.18) if shards else 1.0
    values = jax.random.normal(stream_key, shape, jnp.float32) * scale * level
    return jnp.minimum(jnp.maximum(values, -most), most).astype(kind)


def setup_inputs(seed: int = 0) -> dict:
    streams_of = jax.random.split(jax.random.key(seed), 16)
    return {
        "pair_in": scatter_about(streams_of[0], (L, L, CP), 1.0, 6.0, ((0, 16), (1, 8))),
        "coords": scatter_about(streams_of[1], (3, L), 6.0, 36.0, ((1, 16),), jnp.float32),
        "chain_ids": jnp.searchsorted(jnp.cumsum(ragged(streams_of[2], 4, L, L // 2, 0)), jnp.arange(L), side="right").astype(jnp.int32),
        "coord_mask": with_ends((jax.random.randint(streams_of[3], (L,), 0, 8) < 7).astype(jnp.int32), jax.random.fold_in(streams_of[3], 1), 0, 1),
        "gain_tri": jnp.clip(1.0 + 0.18 * jax.random.normal(streams_of[4], (CP,), jnp.float32), 0.1, 1.9),
        "gain_sum": jnp.clip(1.0 + 0.18 * jax.random.normal(streams_of[5], (CP,), jnp.float32), 0.1, 1.9),
        "gain_attn": jnp.clip(1.0 + 0.18 * jax.random.normal(streams_of[6], (CP,), jnp.float32), 0.1, 1.9),
        "w_tri_in": scatter_about(streams_of[7], (CP, 5 * CP), CP ** -0.5, 0.5),
        "w_tri_out": scatter_about(streams_of[8], (CP, CP), CP ** -0.5, 0.5),
        "w_bins": scatter_about(streams_of[9], (NBINS, CP), 0.5, 3.0, (), jnp.float32),
        "same_chain": scatter_about(streams_of[10], (CP,), 1.0, 6.0, (), jnp.float32),
        "w_query": draw_w_query(jax.random.fold_in(streams_of[15], 71), 0),
        "w_attn": scatter_about(streams_of[12], (CP, 3 * CP), CP ** -0.5, 0.5),
        "w_bias": scatter_about(streams_of[13], (CP, HEADS), CP ** -0.5, 0.5),
        "w_attn_out": scatter_about(streams_of[14], (CP, CP), CP ** -0.5, 0.5),
    }


def layer_norm(values, gain):
    center = values - lax.optimization_barrier(jnp.mean(values, axis=-1, keepdims=True))
    spread = lax.optimization_barrier(jnp.mean(center * center, axis=-1, keepdims=True))
    return center * lax.rsqrt(spread + 1e-05) * gain

def reference(pair_in, coords, chain_ids, coord_mask, gain_tri, gain_sum, gain_attn, w_tri_in, w_tri_out, w_bins, same_chain, w_query, w_attn, w_bias, w_attn_out):
    pair_wide = pair_in.astype(jnp.float32)
    normed = layer_norm(pair_wide, gain_tri).astype(jnp.bfloat16)
    projected = jnp.dot(normed.reshape(L * L, CP), w_tri_in, preferred_element_type=jnp.float32).reshape(L, L, 5 * CP)
    left_side = (jax.nn.sigmoid(projected[..., :CP]) * projected[..., CP:2 * CP]).astype(jnp.bfloat16)
    right_side = (jax.nn.sigmoid(projected[..., 2 * CP:3 * CP]) * projected[..., 3 * CP:4 * CP]).astype(jnp.bfloat16)
    tri_gate = jax.nn.sigmoid(projected[..., 4 * CP:])
    left_first = left_side.astype(jnp.float32).transpose(2, 0, 1)
    right_first = right_side.astype(jnp.float32).transpose(2, 0, 1)
    product = jnp.einsum('cik,cjk->cij', left_first, right_first).transpose(1, 2, 0)
    summed_norm = layer_norm(product, gain_sum).astype(jnp.bfloat16)
    pair_one = pair_wide + tri_gate * jnp.dot(summed_norm.reshape(L * L, CP), w_tri_out, preferred_element_type=jnp.float32).reshape(L, L, CP)
    offsets = coords[:, :, None] - coords[:, None, :]
    dist = jnp.sqrt(lax.optimization_barrier(jnp.sum(offsets * offsets, axis=0)) + 1.0)
    centres = 2.0 + 20.0 * jnp.arange(NBINS, dtype=jnp.float32) / (NBINS - 1)
    spacing = 25.0 / (NBINS - 1)
    present = coord_mask.astype(jnp.float32)
    pair_mask = present[:, None] * present[None, :]
    feats = jnp.exp(-((dist[..., None] - centres) / spacing) ** 2) * pair_mask[..., None]
    binned = jnp.dot(feats.reshape(L * L, NBINS), w_bins, precision=lax.Precision.HIGHEST).reshape(L, L, CP)
    shared = (chain_ids[:, None] == chain_ids[None, :]).astype(jnp.float32)
    pair_two = (pair_one + binned + shared[..., None] * same_chain).astype(jnp.bfloat16)
    normed_two = layer_norm(pair_two.astype(jnp.float32), gain_attn).astype(jnp.bfloat16)
    flat_two = normed_two.reshape(L * L, CP)
    queries = jnp.dot(flat_two, w_query, preferred_element_type=jnp.float32).astype(jnp.bfloat16).reshape(L, L, HEADS, HEAD_DIM)
    rest = jnp.dot(flat_two, w_attn, preferred_element_type=jnp.float32).reshape(L, L, 3 * CP)
    key_rows = rest[..., :CP].astype(jnp.bfloat16).reshape(L, L, HEADS, HEAD_DIM)
    value_rows = rest[..., CP:2 * CP].astype(jnp.bfloat16).reshape(L, L, HEADS, HEAD_DIM)
    attn_gate = jax.nn.sigmoid(rest[..., 2 * CP:])
    pair_bias = jnp.dot(flat_two, w_bias, preferred_element_type=jnp.float32).astype(jnp.bfloat16).reshape(L, L, HEADS)
    bias_first = pair_bias.astype(jnp.float32).transpose(2, 0, 1)
    group = math.gcd(L, 16)
    blocks = L // group

    def one_block(items):
        query_blk, key_blk, value_blk = items
        scores = jnp.einsum('ijhd,ikhd->ihjk', query_blk.astype(jnp.float32), key_blk.astype(jnp.float32)) / math.sqrt(HEAD_DIM) + bias_first[None]
        top = lax.optimization_barrier(jnp.max(scores, axis=-1, keepdims=True))
        expo = jnp.exp(scores - top)
        weights = lax.optimization_barrier(expo.astype(jnp.bfloat16)).astype(jnp.float32)
        numer = jnp.einsum('ihjk,ikhd->ihjd', weights, value_blk.astype(jnp.float32))
        return numer / lax.optimization_barrier(jnp.sum(expo, axis=-1))[..., None]
    attended = lax.map(one_block, (queries.reshape(blocks, group, L, HEADS, HEAD_DIM), key_rows.reshape(blocks, group, L, HEADS, HEAD_DIM), value_rows.reshape(blocks, group, L, HEADS, HEAD_DIM)))
    attended = attended.reshape(L, HEADS, L, HEAD_DIM).transpose(0, 2, 1, 3).reshape(L, L, CP)
    gated = (attn_gate * attended).astype(jnp.bfloat16)
    result = pair_two.astype(jnp.float32) + jnp.dot(gated.reshape(L * L, CP), w_attn_out, preferred_element_type=jnp.float32).reshape(L, L, CP)
    return result.astype(jnp.bfloat16)
```

```python
import functools
import math

import jax
import jax.numpy as jnp
from jax import lax
from jax.experimental import pallas as pl
from jax.experimental.pallas import tpu as pltpu
from jax.sharding import Mesh
from jax.sharding import PartitionSpec as P

BF = jnp.bfloat16
F32 = jnp.float32
LOG2E = 1.4426950408889634


def layer_norm(values, gain):
    center = values - jnp.mean(values, axis=-1, keepdims=True)
    spread = jnp.mean(center * center, axis=-1, keepdims=True)
    return center * lax.rsqrt(spread + 1e-05) * gain


def dot(a, b):
    return jnp.dot(a, b, preferred_element_type=F32)


def exchange(x, axes):
    return lax.all_to_all(x, axes, split_axis=0, concat_axis=0, tiled=True)


def attention_kernel(
    own_ref, full_ref, two_ref, bias_ref, wq_ref, wkv_ref, wg_ref, wo_ref, out_ref, bias_sc
):
    n_heads, n_q, n_k = bias_sc.shape
    channels = own_ref.shape[-1]
    head = channels // n_heads
    step = 128

    @pl.when(pl.program_id(0) == 0)
    def _():
        for h in range(n_heads):
            bias_sc[h] = bias_ref[h].astype(F32) * LOG2E

    own = own_ref[0]
    q = dot(own, wq_ref[...]).astype(BF)
    kv = dot(full_ref[0], wkv_ref[...]).astype(BF)
    k = kv[:, :channels]
    v = jnp.concatenate([kv[:, channels:], jnp.ones((n_k, channels), BF)], axis=1)
    lane_head = lax.broadcasted_iota(jnp.int32, (step, channels), 1) // head
    scale = LOG2E / math.sqrt(head)
    for t in range(n_q // step):
        rows = slice(t * step, (t + 1) * step)
        acc = jnp.zeros((step, channels), F32)
        for h in range(n_heads):
            mine = lane_head == h
            qm = jnp.where(mine, q[rows], jnp.zeros((), BF))
            s = lax.dot_general(qm, k, (((1,), (1,)), ((), ())), preferred_element_type=F32)
            s = s * scale + bias_sc[h, rows, :]
            top = jnp.max(s, axis=-1, keepdims=True)
            p = jnp.exp2(s - top).astype(BF)
            o = dot(p, v)
            acc = jnp.where(mine, o[:, :channels] / o[:, channels:], acc)
        gate = jax.nn.sigmoid(dot(own[rows], wg_ref[...]))
        gated = (gate * acc).astype(BF)
        res = two_ref[0, rows, :].astype(F32) + dot(gated, wo_ref[...])
        out_ref[0, rows, :] = res.astype(BF)


def attention(own, full, two, bias, wq, wkv, wg, wo):
    n_rows, n_q, channels = own.shape
    n_k = full.shape[1]
    n_heads = bias.shape[0]
    row = lambda i: (i, 0, 0)
    fixed2 = lambda i: (0, 0)
    return pl.pallas_call(
        attention_kernel,
        grid=(n_rows,),
        in_specs=[
            pl.BlockSpec((1, n_q, channels), row),
            pl.BlockSpec((1, n_k, channels), row),
            pl.BlockSpec((1, n_q, channels), row),
            pl.BlockSpec(bias.shape, lambda i: (0, 0, 0)),
            pl.BlockSpec(wq.shape, fixed2),
            pl.BlockSpec(wkv.shape, fixed2),
            pl.BlockSpec(wg.shape, fixed2),
            pl.BlockSpec(wo.shape, fixed2),
        ],
        out_specs=pl.BlockSpec((1, n_q, channels), row),
        out_shape=jax.ShapeDtypeStruct(own.shape, BF),
        scratch_shapes=[pltpu.VMEM((n_heads, n_q, n_k), F32)],
        name="attention",
    )(own, full, two, bias, wq, wkv, wg, wo)


def body(
    pair_in,
    coords,
    chain_ids,
    coord_mask,
    gain_tri,
    gain_sum,
    gain_attn,
    w_tri_in,
    w_tri_out,
    w_bins,
    same_chain,
    w_query,
    w_attn,
    w_bias,
    w_attn_out,
):
    n_rh, n_core, n_col = (lax.axis_size(a) for a in ("rh", "core", "col"))
    rh, core, col = (lax.axis_index(a) for a in ("rh", "core", "col"))
    n_dev = n_rh * n_core * n_col
    every = ("rh", "core", "col")
    row_count, col_count, ch = pair_in.shape
    n_heads = w_bias.shape[1]
    n_bins = w_bins.shape[0]
    sub = row_count // n_col
    half = col_count // n_core
    total = n_rh * n_core * row_count
    n_pa = n_core * sub
    n_q = n_col * half

    moved = exchange(
        pair_in.reshape(sub, n_col, n_core, half, ch)
        .transpose(2, 1, 0, 3, 4)
        .reshape(n_core * n_col, sub, half, ch),
        ("core", "col"),
    )
    pair_c = (
        moved.reshape(n_core, n_col, sub, half, ch).transpose(0, 2, 1, 3, 4).reshape(n_pa, n_q, ch)
    )

    packed = jnp.concatenate(
        [coords, chain_ids.astype(F32)[None], coord_mask.astype(F32)[None]], axis=0
    )
    known = exchange(
        jnp.broadcast_to(packed, (n_rh * n_core, *packed.shape)), ("rh", "core")
    ).reshape(n_rh, n_core, -1, row_count)

    normed = layer_norm(pair_in.astype(F32), gain_tri).astype(BF).reshape(-1, ch)
    proj = dot(normed, w_tri_in[:, : 4 * ch])
    left = (jax.nn.sigmoid(proj[:, :ch]) * proj[:, ch : 2 * ch]).astype(BF)
    right = (jax.nn.sigmoid(proj[:, 2 * ch : 3 * ch]) * proj[:, 3 * ch :]).astype(BF)
    both = jnp.stack([left, right], axis=0).reshape(2, row_count, col_count, ch)
    sides = exchange(both.transpose(3, 0, 1, 2), every).reshape(
        n_rh, n_core, n_col, 2, row_count, col_count
    )
    left_k = sides[:, :, :, 0].transpose(0, 1, 3, 2, 4).reshape(total, total)
    right_k = sides[:, :, :, 1].transpose(1, 0, 3, 2, 4).reshape(total, total)
    product = lax.dot_general(
        left_k, right_k, (((1,), (1,)), ((), ())), preferred_element_type=F32
    ).astype(BF)
    lanes = 128
    n_lt = n_q // lanes
    back = exchange(
        product.reshape(n_rh, n_pa, n_col, n_core, n_lt, lanes)
        .transpose(0, 3, 2, 4, 1, 5)
        .reshape(n_dev, n_lt * n_pa, lanes),
        every,
    )
    product_c = (
        back.reshape(ch, n_lt, n_pa, lanes).transpose(2, 1, 3, 0).reshape(n_pa, n_q, ch).astype(F32)
    )
    summed = layer_norm(product_c, gain_sum).astype(BF)
    wide_c = pair_c.astype(F32)
    normed_c = layer_norm(wide_c, gain_tri).astype(BF).reshape(-1, ch)
    tri_gate = jax.nn.sigmoid(dot(normed_c, w_tri_in[:, 4 * ch :]))
    pair_one = wide_c + (tri_gate * dot(summed.reshape(-1, ch), w_tri_out)).reshape(n_pa, n_q, ch)

    near = lax.dynamic_index_in_dim(known, rh, 0, keepdims=False)
    near = near.transpose(1, 0, 2).reshape(-1, n_core, sub, n_col)
    near = lax.dynamic_index_in_dim(near, col, 3, keepdims=False).reshape(-1, n_pa)
    far = lax.dynamic_index_in_dim(known, core, 1, keepdims=False)
    far = far.transpose(1, 0, 2).reshape(-1, n_q)
    offsets = near[:3, :, None] - far[:3, None, :]
    dist = jnp.sqrt(jnp.sum(offsets * offsets, axis=0) + 1.0)
    centres = 2.0 + 20.0 * jnp.arange(n_bins, dtype=F32) / (n_bins - 1)
    spacing = 25.0 / (n_bins - 1)
    pair_mask = near[4][:, None] * far[4][None, :]
    feats = jnp.exp(-(((dist[..., None] - centres) / spacing) ** 2)) * pair_mask[..., None]
    binned = jnp.dot(feats.reshape(-1, n_bins), w_bins).reshape(n_pa, n_q, ch)
    shared = (near[3][:, None] == far[3][None, :]).astype(F32)
    pair_two = (pair_one + binned + shared[..., None] * same_chain).astype(BF)
    normed_two = layer_norm(pair_two.astype(F32), gain_attn).astype(BF)

    flat_two = normed_two.reshape(-1, ch)
    bias = (
        lax.dot_general(w_bias, flat_two, (((0,), (1,)), ((), ())), preferred_element_type=F32)
        .astype(BF)
        .reshape(n_heads, n_core, sub, n_q)
        .transpose(1, 0, 2, 3)
        .reshape(n_core, n_heads * sub, n_q)
    )
    spread = exchange(
        jnp.broadcast_to(
            bias[None, :, None], (n_rh, n_core, n_col, n_heads * sub, n_q)
        ).reshape(n_dev, n_heads * sub, n_q),
        every,
    )
    bias_c = (
        spread.reshape(n_rh, n_core, n_col, n_heads, sub, n_q)
        .transpose(3, 0, 4, 2, 1, 5)
        .reshape(n_heads, n_q, n_core * n_q)
    )

    order = [(d, d ^ n_col) for d in range(n_dev)]
    other = lax.ppermute(normed_two, every, order)
    full = jnp.where(
        core == 0,
        jnp.concatenate([normed_two, other], axis=1),
        jnp.concatenate([other, normed_two], axis=1),
    )
    result = attention(
        normed_two,
        full,
        pair_two,
        bias_c,
        w_query,
        w_attn[:, : 2 * ch],
        w_attn[:, 2 * ch :],
        w_attn_out,
    )
    home = exchange(
        result.reshape(n_core, sub, n_col, half, ch)
        .transpose(0, 2, 1, 3, 4)
        .reshape(n_core * n_col, sub, half, ch),
        ("core", "col"),
    )
    return (
        home.reshape(n_core, n_col, sub, half, ch)
        .transpose(2, 1, 0, 3, 4)
        .reshape(row_count, col_count, ch)
    )


def solution(mesh):
    n_row, n_col = mesh.shape["row"], mesh.shape["col"]
    split = Mesh(mesh.devices.reshape(n_row // 2, 2, n_col), ("rh", "core", "col"))
    row = ("rh", "core")
    return jax.shard_map(
        body,
        mesh=split,
        in_specs=(P(row, "col", None), P(None, row), P(row), P(row)) + (P(),) * 11,
        out_specs=P(row, "col", None),
        check_vma=False,
    )
```

```python
import functools
import math

import jax
import jax.numpy as jnp
from jax import lax
from jax.experimental import pallas as pl
from jax.experimental.pallas import tpu as pltpu
from jax.sharding import Mesh
from jax.sharding import PartitionSpec as P

BF = jnp.bfloat16
F32 = jnp.float32
LOG2E = 1.4426950408889634
NT = (((1,), (1,)), ((), ()))
LANES = 128


def layer_norm(values, gain):
    center = values - jnp.mean(values, axis=-1, keepdims=True)
    spread = jnp.mean(center * center, axis=-1, keepdims=True)
    return center * lax.rsqrt(spread + 1e-05) * gain


def dot(a, b):
    return jnp.dot(a, b, preferred_element_type=F32)


def dot_nt(a, b):
    return lax.dot_general(a, b, NT, preferred_element_type=F32)


def exchange(x, axes):
    return lax.all_to_all(x, axes, split_axis=0, concat_axis=0, tiled=True)


def sides_kernel(x_ref, gain_ref, w_ref, out_ref, norm_sc, sc):
    n_rows, n_cols, ch = x_ref.shape
    n_out = out_ref.shape[1]
    third = n_rows // 3
    cut = LANES - n_cols

    def norm(i, carry):
        for u in range(4):
            norm_sc[i * 4 + u] = layer_norm(x_ref[i * 4 + u].astype(F32), gain_ref[...]).astype(BF)
        return carry

    lax.fori_loop(0, n_rows // 4, norm, 0)

    def sides(x):
        pr = dot_nt(w_ref[...], x)
        left = jax.nn.sigmoid(pr[:ch]) * pr[ch : 2 * ch]
        right = jax.nn.sigmoid(pr[2 * ch : 3 * ch]) * pr[3 * ch :]
        return left, right

    def put(row, value):
        sc[pl.ds(row, ch, stride=n_out), :] = value

    def main(s, carry):
        x = jnp.concatenate(
            [
                norm_sc[s],
                norm_sc[third + s, :cut],
                norm_sc[2 * third + s],
                norm_sc[third + s, cut : 2 * cut],
            ],
            axis=0,
        )
        left, right = sides(x)
        put(s, left[:, :LANES])
        put(third + s, left[:, LANES:])
        put(2 * third + s, right[:, :LANES])
        put(3 * third + s, right[:, LANES:])
        return carry

    lax.fori_loop(0, third, main, 0)

    is_left = lax.broadcasted_iota(jnp.int32, (ch, LANES), 1) < LANES // 2

    def rest(s, carry):
        one = norm_sc[third + s, 2 * cut :]
        two = norm_sc[third + third // 2 + s, 2 * cut :]
        left, right = sides(jnp.concatenate([one, two, one, two], axis=0))
        put(4 * third + s, jnp.where(is_left, left, right))
        return carry

    lax.fori_loop(0, third // 2, rest, 0)

    def emit(c, carry):
        out_ref[c] = sc[pl.ds(pl.multiple_of(c * n_out, 8), n_out), :].astype(BF)
        return carry

    lax.fori_loop(0, ch, emit, 0)


def make_sides(pair, gain, w_t):
    n_rows, n_cols, ch = pair.shape
    n_out = 2 * n_rows * n_cols // LANES
    return pl.pallas_call(
        sides_kernel,
        out_shape=jax.ShapeDtypeStruct((ch, n_out, LANES), BF),
        scratch_shapes=[
            pltpu.VMEM(pair.shape, BF),
            pltpu.VMEM((ch * n_out, LANES), F32),
        ],
        name="sides",
    )(pair, gain.reshape(1, ch), w_t)


def triangle_kernel(n_rh, n_core, n_col, n_rows, n_cols, in_ref, out_ref, l_sc, r_sc, p_sc):
    third = n_rows // 3
    cut = LANES - n_cols
    total = n_rh * n_core * n_rows
    n_pa = n_core * n_rows // n_col
    n_lt = total // n_core // LANES
    lane = lax.broadcasted_iota(jnp.int32, (third, LANES), 1)

    def middle(a, b, c):
        return jnp.where(
            lane < cut,
            pltpu.roll(a, cut, 1),
            jnp.where(lane < 2 * cut, pltpu.roll(b, 2 * cut, 1), jnp.where(lane < n_cols, c, 0.0)),
        )

    def unpack(rh, carry):
        for p in range(n_core):
            for c in range(n_col):
                blk = in_ref[(rh * n_core + p) * n_col + c].astype(F32)
                b = [blk[third * t : third * (t + 1)] for t in range(4)]
                last = blk[4 * third :]
                keep = [jnp.where(lane < n_cols, t, 0.0) for t in b]
                lc = jnp.concatenate([pltpu.roll(last, 2 * cut, 1), pltpu.roll(last, cut, 1)], axis=0)
                rc = jnp.concatenate([last, pltpu.roll(last, 3 * cut, 1)], axis=0)
                left = jnp.concatenate([keep[0], middle(b[0], b[1], lc), keep[1]], axis=0)
                right = jnp.concatenate([keep[2], middle(b[2], b[3], rc), keep[3]], axis=0)
                lanes = slice(c * LANES, (c + 1) * LANES)
                at_l = pl.multiple_of((rh * n_core + p) * n_rows, 16)
                at_r = pl.multiple_of((p * n_rh + rh) * n_rows, 16)
                l_sc[pl.ds(at_l, n_rows), lanes] = left.astype(BF)
                r_sc[pl.ds(at_r, n_rows), lanes] = right.astype(BF)
        return carry

    lax.fori_loop(0, n_rh, unpack, 0)
    wide = 2 * LANES
    for t in range(total // wide):
        part = dot_nt(l_sc[...], r_sc[t * wide : (t + 1) * wide, :])
        p_sc[2 * t] = part[:, :LANES]
        p_sc[2 * t + 1] = part[:, LANES:]

    def pack(rh, carry):
        for core in range(n_core):
            for c in range(n_col):
                rows = pl.ds(rh * n_core * n_rows + c, n_pa, stride=n_col)
                parts = [p_sc[core * n_lt + t, rows, :] for t in range(n_lt)]
                out_ref[(rh * n_core + core) * n_col + c] = jnp.concatenate(parts, axis=0).astype(BF)
        return carry

    lax.fori_loop(0, n_rh, pack, 0)


def triangle(sides, n_rh, n_core, n_col, n_rows, n_cols):
    total = n_rh * n_core * n_rows
    n_pa = n_core * n_rows // n_col
    n_lt = total // n_core // LANES
    return pl.pallas_call(
        functools.partial(triangle_kernel, n_rh, n_core, n_col, n_rows, n_cols),
        out_shape=jax.ShapeDtypeStruct((sides.shape[0], n_lt * n_pa, LANES), BF),
        scratch_shapes=[
            pltpu.VMEM((total, n_col * LANES), BF),
            pltpu.VMEM((total, n_col * LANES), BF),
            pltpu.VMEM((total // LANES, total, LANES), F32),
        ],
        name="triangle",
    )(sides)


def update_kernel(
    n_bins,
    back_ref,
    pair_ref,
    near_ref,
    far_ref,
    gain_tri_ref,
    gain_sum_ref,
    gain_attn_ref,
    wgo_ref,
    wout_ref,
    wbins_ref,
    same_ref,
    wbias_ref,
    two_ref,
    normed_ref,
    bias_ref,
    sc,
):
    ch, n_in, _ = back_ref.shape
    n_q = far_ref.shape[0]
    n_lt = n_q // LANES
    n_pa = n_in // n_lt
    n_in8 = sc.shape[0] // ch
    sub = pair_ref.shape[2]
    pa = pl.program_id(0)
    n_heads = bias_ref.shape[1]

    @pl.when(pa == 0)
    def _():
        def widen(c, carry):
            sc[pl.ds(pl.multiple_of(c * n_in8, 8), n_in), :] = back_ref[c].astype(F32)
            return carry

        lax.fori_loop(0, ch, widen, 0)

    parts = []
    for t in range(n_lt):
        x = sc[pl.ds(t * n_pa + pa, ch, stride=n_in8), :]
        center = x - jnp.mean(x, axis=0, keepdims=True)
        spread = jnp.mean(center * center, axis=0, keepdims=True)
        summed = (center * lax.rsqrt(spread + 1e-05) * gain_sum_ref[...]).astype(BF)
        parts.append(
            lax.dot_general(
                summed, wout_ref[...], (((0,), (0,)), ((), ())), preferred_element_type=F32
            )
        )
    tri = jnp.concatenate(parts, axis=0)
    wide = pair_ref[0, :, 0].reshape(n_q, ch).astype(F32)
    gate = jax.nn.sigmoid(dot(layer_norm(wide, gain_tri_ref[...]).astype(BF), wgo_ref[...]))
    far = far_ref[...]
    near = [near_ref[f, pa] for f in range(5)]
    square = jnp.zeros((n_q, 1), F32)
    for f in range(3):
        off = far[:, f : f + 1] - near[f]
        square = square + off * off
    dist = jnp.sqrt(square + 1.0)
    bins = lax.broadcasted_iota(jnp.int32, (1, ch), 1).astype(F32)
    centres = 2.0 + 20.0 * bins / (n_bins - 1)
    z = (dist - centres) * ((n_bins - 1) / 25.0)
    feats = jnp.exp(-(z * z)) * (far[:, 4:5] * near[4])
    binned = dot(feats, wbins_ref[...])
    shared = (far[:, 3:4] == near[3]).astype(F32)
    two = (wide + gate * tri + binned + shared * same_ref[...]).astype(BF)
    two_ref[0] = two
    normed = layer_norm(two.astype(F32), gain_attn_ref[...]).astype(BF)
    normed_ref[0] = normed
    bias_ref[0] = dot_nt(wbias_ref[...], normed)[:n_heads].astype(BF)


def update(back, moved, near, far, gains, wgo, wout, wbins, same, wbias_t, n_heads, n_bins):
    ch, n_in, _ = back.shape
    n_core, n_col, sub, half, _ = moved.shape
    n_q = n_col * half
    n_pa = n_core * sub
    n_in8 = -(-n_in // 8) * 8
    fixed = lambda i: (0, 0)
    row = lambda i: (i, 0, 0)
    return pl.pallas_call(
        functools.partial(update_kernel, n_bins),
        grid=(n_pa,),
        in_specs=[
            pl.BlockSpec(back.shape, lambda i: (0, 0, 0)),
            pl.BlockSpec((1, n_col, 1, half, ch), lambda i: (i // sub, 0, i % sub, 0, 0)),
            pl.BlockSpec(memory_space=pltpu.SMEM),
            pl.BlockSpec(far.shape, fixed),
            pl.BlockSpec((1, ch), fixed),
            pl.BlockSpec((ch, 1), fixed),
            pl.BlockSpec((1, ch), fixed),
            pl.BlockSpec(wgo.shape, fixed),
            pl.BlockSpec(wout.shape, fixed),
            pl.BlockSpec(wbins.shape, fixed),
            pl.BlockSpec(same.shape, fixed),
            pl.BlockSpec(wbias_t.shape, fixed),
        ],
        out_specs=[
            pl.BlockSpec((1, n_q, ch), row),
            pl.BlockSpec((1, n_q, ch), row),
            pl.BlockSpec((1, n_heads, n_q), row),
        ],
        out_shape=[
            jax.ShapeDtypeStruct((n_pa, n_q, ch), BF),
            jax.ShapeDtypeStruct((n_pa, n_q, ch), BF),
            jax.ShapeDtypeStruct((n_pa, n_heads, n_q), BF),
        ],
        scratch_shapes=[pltpu.VMEM((ch * n_in8, LANES), F32)],
        name="update",
    )(back, moved, near, far, gains[0], gains[1], gains[2], wgo, wout, wbins, same, wbias_t)


def attention_kernel(
    core_ref,
    own_ref,
    other_ref,
    two_ref,
    bias_ref,
    wq_ref,
    wkv_ref,
    wg_ref,
    wo_ref,
    out_ref,
    raw_sc,
    bias_sc,
    kv_sc,
):
    n_lt, tall, n_k = bias_sc.shape
    n_q, channels = own_ref.shape[1:]
    n_heads = tall // LANES
    n_src, n_pay, _ = bias_ref.shape
    sub = n_pay // n_heads
    n_col = n_q // sub // (n_src // 16)
    head = channels // n_heads

    @pl.when(pl.program_id(0) == 0)
    def _():
        def widen(d, carry):
            for t in range(n_lt):
                part = bias_ref[d, :, t * LANES : (t + 1) * LANES]
                raw_sc[t, pl.ds(pl.multiple_of(d * n_pay, 8), n_pay), :] = part.astype(F32) * LOG2E
            return carry

        lax.fori_loop(0, n_src, widen, 0)
        n_rh = n_src // 2 // n_col
        for rh in range(n_rh):
            for a in range(sub):
                q0 = rh * sub * n_col + a * n_col
                t, q1 = q0 // LANES, q0 % LANES
                for s in range(2):
                    for h in range(n_heads):
                        for u in range(n_lt):
                            at = (rh * 2 + s) * n_col * n_pay + a * n_heads + h
                            bias_sc[
                                t,
                                h * LANES + q1 : h * LANES + q1 + n_col,
                                s * n_q + u * LANES : s * n_q + (u + 1) * LANES,
                            ] = raw_sc[u, pl.ds(at, n_col, stride=n_pay), :]

    core = core_ref[0]
    own = own_ref[0]
    q = dot(own, wq_ref[...]).astype(BF)
    kv_sc[pl.ds(pl.multiple_of(core * n_q, LANES), n_q), : 2 * channels] = dot(
        own, wkv_ref[...]
    ).astype(BF)
    kv_sc[pl.ds(pl.multiple_of((1 - core) * n_q, LANES), n_q), : 2 * channels] = dot(
        other_ref[0], wkv_ref[...]
    ).astype(BF)
    kv_sc[:, 2 * channels :] = jnp.ones((n_k, channels), BF)
    k = kv_sc[:, :channels]
    v = kv_sc[:, channels:]
    lane_head = lax.broadcasted_iota(jnp.int32, (LANES, channels), 1) // head
    scale = LOG2E / math.sqrt(head)
    zero = jnp.zeros((), BF)

    def scores(t):
        rows = q[t * LANES : (t + 1) * LANES]
        tall_q = jnp.concatenate(
            [jnp.where(lane_head == h, rows, zero) for h in range(n_heads)], axis=0
        )
        return dot_nt(tall_q, k)

    s = scores(0)
    for t in range(n_lt):
        ahead = scores(t + 1) if t + 1 < n_lt else None
        s = s * scale + bias_sc[t]
        p = jnp.exp2(s - jnp.max(s, axis=-1, keepdims=True)).astype(BF)
        o = dot(p, v)
        acc = jnp.zeros((LANES, channels), F32)
        for h in range(n_heads):
            part = o[h * LANES : (h + 1) * LANES]
            acc = jnp.where(lane_head == h, part[:, :channels] / part[:, channels:], acc)
        rows = slice(t * LANES, (t + 1) * LANES)
        gate = jax.nn.sigmoid(dot(own[rows], wg_ref[...]))
        gated = (gate * acc).astype(BF)
        res = two_ref[0, rows, :].astype(F32) + dot(gated, wo_ref[...])
        out_ref[0, rows, :] = res.astype(BF)
        s = ahead


def attention(core, own, other, two, bias, wq, wkv, wg, wo, n_heads):
    n_rows, n_q, channels = own.shape
    n_src, n_pay, _ = bias.shape
    n_lt = n_q // LANES
    row = lambda i: (i, 0, 0)
    fixed2 = lambda i: (0, 0)
    return pl.pallas_call(
        attention_kernel,
        grid=(n_rows,),
        in_specs=[
            pl.BlockSpec(memory_space=pltpu.SMEM),
            pl.BlockSpec((1, n_q, channels), row),
            pl.BlockSpec((1, n_q, channels), row),
            pl.BlockSpec((1, n_q, channels), row),
            pl.BlockSpec(bias.shape, lambda i: (0, 0, 0)),
            pl.BlockSpec(wq.shape, fixed2),
            pl.BlockSpec(wkv.shape, fixed2),
            pl.BlockSpec(wg.shape, fixed2),
            pl.BlockSpec(wo.shape, fixed2),
        ],
        out_specs=pl.BlockSpec((1, n_q, channels), row),
        out_shape=jax.ShapeDtypeStruct(own.shape, BF),
        scratch_shapes=[
            pltpu.VMEM((n_lt, n_src * n_pay, LANES), F32),
            pltpu.VMEM((n_lt, n_heads * LANES, 2 * n_q), F32),
            pltpu.VMEM((2 * n_q, 3 * channels), BF),
        ],
        name="attention",
    )(core, own, other, two, bias, wq, wkv, wg, wo)


def body(
    pair_in,
    coords,
    chain_ids,
    coord_mask,
    gain_tri,
    gain_sum,
    gain_attn,
    w_tri_in,
    w_tri_out,
    w_bins,
    same_chain,
    w_query,
    w_attn,
    w_bias,
    w_attn_out,
):
    n_rh, n_core, n_col = (lax.axis_size(a) for a in ("rh", "core", "col"))
    rh, core, col = (lax.axis_index(a) for a in ("rh", "core", "col"))
    n_dev = n_rh * n_core * n_col
    every = ("rh", "core", "col")
    row_count, col_count, ch = pair_in.shape
    n_heads = w_bias.shape[1]
    n_bins = w_bins.shape[0]
    sub = row_count // n_col
    half = col_count // n_core
    n_pa = n_core * sub
    n_q = n_col * half

    moved = exchange(
        pair_in.reshape(sub, n_col, n_core, half, ch)
        .transpose(2, 1, 0, 3, 4)
        .reshape(n_core * n_col, sub, half, ch),
        ("core", "col"),
    ).reshape(n_core, n_col, sub, half, ch)

    packed = jnp.concatenate(
        [coords, chain_ids.astype(F32)[None], coord_mask.astype(F32)[None]], axis=0
    )
    known = exchange(
        jnp.broadcast_to(packed, (n_rh * n_core, *packed.shape)), ("rh", "core")
    ).reshape(n_rh, n_core, -1, row_count)
    near = lax.dynamic_index_in_dim(known, rh, 0, keepdims=False)
    near = near.transpose(1, 0, 2).reshape(-1, n_core, sub, n_col)
    near = lax.dynamic_index_in_dim(near, col, 3, keepdims=False).reshape(-1, n_pa)
    far = lax.dynamic_index_in_dim(known, core, 1, keepdims=False)
    far = far.transpose(0, 2, 1).reshape(n_q, -1)

    sides = exchange(make_sides(pair_in, gain_tri, w_tri_in[:, : 4 * ch].T), every)
    back = exchange(triangle(sides, n_rh, n_core, n_col, row_count, col_count), every)
    two, normed, bias = update(
        back,
        moved,
        near,
        far,
        (gain_tri.reshape(1, ch), gain_sum.reshape(ch, 1), gain_attn.reshape(1, ch)),
        w_tri_in[:, 4 * ch :],
        w_tri_out,
        jnp.pad(w_bins, ((0, ch - n_bins), (0, 0))),
        same_chain.reshape(1, ch),
        jnp.pad(w_bias.T, ((0, 16 - n_heads), (0, 0))),
        n_heads,
        n_bins,
    )

    n_pay = sub * n_heads
    spread = exchange(
        jnp.broadcast_to(
            bias.reshape(1, n_core, 1, n_pay, n_q), (n_rh, n_core, n_col, n_pay, n_q)
        ).reshape(n_dev, n_pay, n_q),
        every,
    )
    other = lax.ppermute(normed, every, [(d, d ^ n_col) for d in range(n_dev)])
    result = attention(
        core.reshape(1),
        normed,
        other,
        two,
        spread,
        w_query,
        w_attn[:, : 2 * ch],
        w_attn[:, 2 * ch :],
        w_attn_out,
        n_heads,
    )
    home = exchange(
        result.reshape(n_core, sub, n_col, half, ch)
        .transpose(0, 2, 1, 3, 4)
        .reshape(n_core * n_col, sub, half, ch),
        ("core", "col"),
    )
    return (
        home.reshape(n_core, n_col, sub, half, ch)
        .transpose(2, 1, 0, 3, 4)
        .reshape(row_count, col_count, ch)
    )


def solution(mesh):
    n_row, n_col = mesh.shape["row"], mesh.shape["col"]
    split = Mesh(mesh.devices.reshape(n_row // 2, 2, n_col), ("rh", "core", "col"))
    row = ("rh", "core")
    return jax.shard_map(
        body,
        mesh=split,
        in_specs=(P(row, "col", None), P(None, row), P(row), P(row)) + (P(),) * 11,
        out_specs=P(row, "col", None),
        check_vma=False,
    )
```

```python
import functools
import math

import jax
import jax.numpy as jnp
from jax import lax
from jax.experimental import pallas as pl
from jax.experimental.pallas import tpu as pltpu
from jax.sharding import Mesh
from jax.sharding import PartitionSpec as P

BF = jnp.bfloat16
F32 = jnp.float32
LOG2E = 1.4426950408889634
NT = (((1,), (1,)), ((), ()))
LANES = 128


def layer_norm(values, gain):
    center = values - jnp.mean(values, axis=-1, keepdims=True)
    spread = jnp.mean(center * center, axis=-1, keepdims=True)
    return center * lax.rsqrt(spread + 1e-05) * gain


def dot(a, b):
    return jnp.dot(a, b, preferred_element_type=F32)


def dot_nt(a, b):
    return lax.dot_general(a, b, NT, preferred_element_type=F32)


def exchange(x, axes):
    return lax.all_to_all(x, axes, split_axis=0, concat_axis=0, tiled=True)


def sides_kernel(x_ref, gain_ref, w_ref, out_ref, norm_sc, sc):
    n_rows, n_cols, ch = x_ref.shape
    n_out = out_ref.shape[1]
    third = n_rows // 3
    cut = LANES - n_cols

    def norm(i, carry):
        for u in range(4):
            norm_sc[i * 4 + u] = layer_norm(x_ref[i * 4 + u].astype(F32), gain_ref[...]).astype(BF)
        return carry

    lax.fori_loop(0, n_rows // 4, norm, 0, unroll=2)

    def sides(x):
        pr = dot_nt(w_ref[...], x)
        left = jax.nn.sigmoid(pr[:ch]) * pr[ch : 2 * ch]
        right = jax.nn.sigmoid(pr[2 * ch : 3 * ch]) * pr[3 * ch :]
        return left, right

    def put(row, value):
        sc[pl.ds(row, ch, stride=n_out), :] = value

    def main(s, carry):
        x = jnp.concatenate(
            [
                norm_sc[s],
                norm_sc[third + s, :cut],
                norm_sc[2 * third + s],
                norm_sc[third + s, cut : 2 * cut],
            ],
            axis=0,
        )
        left, right = sides(x)
        put(s, left[:, :LANES])
        put(third + s, left[:, LANES:])
        put(2 * third + s, right[:, :LANES])
        put(3 * third + s, right[:, LANES:])
        return carry

    lax.fori_loop(0, third, main, 0, unroll=4)

    is_left = lax.broadcasted_iota(jnp.int32, (ch, LANES), 1) < LANES // 2

    def rest(s, carry):
        one = norm_sc[third + s, 2 * cut :]
        two = norm_sc[third + third // 2 + s, 2 * cut :]
        left, right = sides(jnp.concatenate([one, two, one, two], axis=0))
        put(4 * third + s, jnp.where(is_left, left, right))
        return carry

    lax.fori_loop(0, third // 2, rest, 0, unroll=4)

    def emit(c, carry):
        out_ref[c] = sc[pl.ds(pl.multiple_of(c * n_out, 8), n_out), :].astype(BF)
        return carry

    lax.fori_loop(0, ch, emit, 0, unroll=16)


def make_sides(pair, gain, w_t):
    n_rows, n_cols, ch = pair.shape
    n_out = 2 * n_rows * n_cols // LANES
    return pl.pallas_call(
        sides_kernel,
        out_shape=jax.ShapeDtypeStruct((ch, n_out, LANES), BF),
        scratch_shapes=[
            pltpu.VMEM(pair.shape, BF),
            pltpu.VMEM((ch * n_out, LANES), F32),
        ],
        name="sides",
    )(pair, gain.reshape(1, ch), w_t)


def triangle_kernel(n_rh, n_core, n_col, n_rows, n_cols, in_ref, out_ref, l_sc, r_sc, p_sc):
    third = n_rows // 3
    cut = LANES - n_cols
    total = n_rh * n_core * n_rows
    n_pa = n_core * n_rows // n_col
    n_lt = total // n_core // LANES
    lane = lax.broadcasted_iota(jnp.int32, (third, LANES), 1)

    def middle(a, b, c):
        return jnp.where(
            lane < cut,
            pltpu.roll(a, cut, 1),
            jnp.where(lane < 2 * cut, pltpu.roll(b, 2 * cut, 1), jnp.where(lane < n_cols, c, 0.0)),
        )

    def unpack(rh, carry):
        for p in range(n_core):
            for c in range(n_col):
                blk = in_ref[(rh * n_core + p) * n_col + c].astype(F32)
                b = [blk[third * t : third * (t + 1)] for t in range(4)]
                last = blk[4 * third :]
                keep = [jnp.where(lane < n_cols, t, 0.0) for t in b]
                lc = jnp.concatenate([pltpu.roll(last, 2 * cut, 1), pltpu.roll(last, cut, 1)], axis=0)
                rc = jnp.concatenate([last, pltpu.roll(last, 3 * cut, 1)], axis=0)
                left = jnp.concatenate([keep[0], middle(b[0], b[1], lc), keep[1]], axis=0)
                right = jnp.concatenate([keep[2], middle(b[2], b[3], rc), keep[3]], axis=0)
                lanes = slice(c * LANES, (c + 1) * LANES)
                at_l = pl.multiple_of((rh * n_core + p) * n_rows, 16)
                at_r = pl.multiple_of((p * n_rh + rh) * n_rows, 16)
                l_sc[pl.ds(at_l, n_rows), lanes] = left.astype(BF)
                r_sc[pl.ds(at_r, n_rows), lanes] = right.astype(BF)
        return carry

    lax.fori_loop(0, n_rh, unpack, 0)
    wide = 2 * LANES
    for t in range(total // wide):
        part = dot_nt(l_sc[...], r_sc[t * wide : (t + 1) * wide, :])
        p_sc[2 * t] = part[:, :LANES]
        p_sc[2 * t + 1] = part[:, LANES:]

    def pack(rh, carry):
        for core in range(n_core):
            for c in range(n_col):
                rows = pl.ds(rh * n_core * n_rows + c, n_pa, stride=n_col)
                parts = [p_sc[core * n_lt + t, rows, :] for t in range(n_lt)]
                out_ref[(rh * n_core + core) * n_col + c] = jnp.concatenate(parts, axis=0).astype(BF)
        return carry

    lax.fori_loop(0, n_rh, pack, 0)


def triangle(sides, n_rh, n_core, n_col, n_rows, n_cols):
    total = n_rh * n_core * n_rows
    n_pa = n_core * n_rows // n_col
    n_lt = total // n_core // LANES
    return pl.pallas_call(
        functools.partial(triangle_kernel, n_rh, n_core, n_col, n_rows, n_cols),
        out_shape=jax.ShapeDtypeStruct((sides.shape[0], n_lt * n_pa, LANES), BF),
        scratch_shapes=[
            pltpu.VMEM((total, n_col * LANES), BF),
            pltpu.VMEM((total, n_col * LANES), BF),
            pltpu.VMEM((total // LANES, total, LANES), F32),
        ],
        name="triangle",
    )(sides)


def unit_norm(x, ones):
    center = x.astype(F32) - dot(x, ones[: x.shape[1]])
    square = center * center
    high = square.astype(BF)
    low = (square - high.astype(F32)).astype(BF)
    spread = dot(jnp.concatenate([high, low], axis=1), ones)
    return center * lax.rsqrt(spread + 1e-05)


def update_kernel(
    n_bins,
    back_ref,
    pair_ref,
    near_ref,
    far_ref,
    gain_tri_ref,
    gain_sum_ref,
    gain_attn_ref,
    wgo_ref,
    wout_ref,
    wbins_ref,
    wbias_ref,
    two_ref,
    normed_ref,
    bias_ref,
    sc,
):
    ch, n_in, _ = back_ref.shape
    n_q = far_ref.shape[1]
    n_lt = n_q // LANES
    n_pa = n_in // n_lt
    n_in8 = sc.shape[0] // ch
    n_heads = bias_ref.shape[1]
    tn = (((0,), (0,)), ((), ()))

    @pl.when(pl.program_id(0) == 0)
    def _():
        def widen(c, carry):
            sc[pl.ds(pl.multiple_of(c * n_in8, 8), n_in), :] = back_ref[c].astype(F32)
            return carry

        lax.fori_loop(0, ch, widen, 0, unroll=16)

    ones = jnp.full((2 * ch, ch), 1.0 / ch, BF)
    n_row = two_ref.shape[0]
    n_feat = wbins_ref.shape[0] // 3
    bin_at = lax.broadcasted_iota(jnp.int32, (n_feat, 1), 0)
    centres = 2.0 + 20.0 * bin_at.astype(F32) / (n_bins - 1)
    parts = []
    pairs = []
    feats = []
    for v in range(n_row):
        pa = pl.program_id(0) * n_row + v
        for t in range(n_lt):
            x = sc[pl.ds(t * n_pa + pa, ch, stride=n_in8), :]
            center = x - jnp.mean(x, axis=0, keepdims=True)
            spread = jnp.mean(center * center, axis=0, keepdims=True)
            parts.append((center * lax.rsqrt(spread + 1e-05) * gain_sum_ref[...]).astype(BF))
        pairs.append(pair_ref[0, :, v].reshape(n_q, ch))
        square = jnp.zeros((1, n_q), F32)
        for f in range(3):
            off = far_ref[f : f + 1, :] - near_ref[f, pa]
            square = square + off * off
        shared = (far_ref[3:4, :] == near_ref[3, pa]).astype(F32)
        mask = far_ref[4:5, :] * near_ref[4, pa]
        z = (jnp.sqrt(square + 1.0) - centres) * ((n_bins - 1) / 25.0)
        bins = jnp.exp(-(z * z)) * mask
        feats.append(jnp.where(bin_at < n_bins, bins, jnp.where(bin_at == n_bins, shared, 0.0)))
    tri = lax.dot_general(
        jnp.concatenate(parts, axis=1), wout_ref[...], tn, preferred_element_type=F32
    )
    pair = jnp.concatenate(pairs, axis=0)
    normed_pair = (unit_norm(pair, ones) * gain_tri_ref[...]).astype(BF)
    gate = jax.nn.sigmoid(dot(normed_pair, wgo_ref[...]))
    feats = jnp.concatenate(feats, axis=1)
    high = feats.astype(BF)
    low = (feats - high.astype(F32)).astype(BF)
    binned = lax.dot_general(
        jnp.concatenate([high, low, high], axis=0), wbins_ref[...], tn, preferred_element_type=F32
    )
    two = (pair.astype(F32) + gate * tri + binned).astype(BF)
    normed = (unit_norm(two, ones) * gain_attn_ref[...]).astype(BF)
    bias = dot_nt(wbias_ref[...], normed)[:n_heads].astype(BF)
    for v in range(n_row):
        two_ref[v] = two[v * n_q : (v + 1) * n_q]
        normed_ref[v] = normed[v * n_q : (v + 1) * n_q]
        bias_ref[v] = bias[:, v * n_q : (v + 1) * n_q]


def bin_weights(w_bins, same_chain):
    n_feat = -(-(w_bins.shape[0] + 1) // 16) * 16
    rows = jnp.concatenate([w_bins, same_chain[None]], axis=0)
    rows = jnp.pad(rows, ((0, n_feat - rows.shape[0]), (0, 0)))
    high = lax.reduce_precision(rows, 8, 7)
    return jnp.concatenate([high, high, rows - high], axis=0).astype(BF)


def update(back, moved, near, far, gains, wgo, wout, wbins, wbias_t, n_heads, n_bins, n_row=6):
    ch, n_in, _ = back.shape
    n_core, n_col, sub, half, _ = moved.shape
    n_q = n_col * half
    n_pa = n_core * sub
    n_in8 = -(-n_in // 8) * 8
    per = sub // n_row
    fixed = lambda i: (0, 0)
    row = lambda i: (i, 0, 0)
    return pl.pallas_call(
        functools.partial(update_kernel, n_bins),
        grid=(n_pa // n_row,),
        in_specs=[
            pl.BlockSpec(back.shape, lambda i: (0, 0, 0)),
            pl.BlockSpec((1, n_col, n_row, half, ch), lambda i: (i // per, 0, i % per, 0, 0)),
            pl.BlockSpec(memory_space=pltpu.SMEM),
            pl.BlockSpec(far.shape, fixed),
            pl.BlockSpec((1, ch), fixed),
            pl.BlockSpec((ch, 1), fixed),
            pl.BlockSpec((1, ch), fixed),
            pl.BlockSpec(wgo.shape, fixed),
            pl.BlockSpec(wout.shape, fixed),
            pl.BlockSpec(wbins.shape, fixed),
            pl.BlockSpec(wbias_t.shape, fixed),
        ],
        out_specs=[
            pl.BlockSpec((n_row, n_q, ch), row),
            pl.BlockSpec((n_row, n_q, ch), row),
            pl.BlockSpec((n_row, n_heads, n_q), row),
        ],
        out_shape=[
            jax.ShapeDtypeStruct((n_pa, n_q, ch), BF),
            jax.ShapeDtypeStruct((n_pa, n_q, ch), BF),
            jax.ShapeDtypeStruct((n_pa, n_heads, n_q), BF),
        ],
        scratch_shapes=[pltpu.VMEM((ch * n_in8, LANES), F32)],
        name="update",
    )(back, moved, near, far, gains[0], gains[1], gains[2], wgo, wout, wbins, wbias_t)


def project_kernel(
    core_ref, own_ref, other_ref, wq_ref, wk_ref, wv_ref, wg_ref, q_ref, k_ref, vt_ref, gate_ref
):
    n_heads, tall, n_k = vt_ref.shape[1:]
    head = wv_ref.shape[0] // n_heads
    first = core_ref[0] == 0
    n_row, n_q, ch = own_ref.shape
    own, other = own_ref[...], other_ref[...]
    full = jnp.concatenate(
        [jnp.where(first, own, other), jnp.where(first, other, own)], axis=1
    ).reshape(n_row * n_k, ch)
    own = own.reshape(n_row * n_q, ch)
    scale = LOG2E / math.sqrt(head)
    q_ref[...] = (dot(own, wq_ref[...]) * scale).astype(BF).reshape(n_row, n_q, ch)
    gate = jax.nn.sigmoid(dot_nt(wg_ref[...], own))
    k_ref[...] = dot(full, wk_ref[...]).astype(BF).reshape(n_row, n_k, ch)
    v_t = dot_nt(wv_ref[...], full).astype(BF)
    for r in range(n_row):
        gate_ref[r] = gate[:, r * n_q : (r + 1) * n_q]
        for h in range(n_heads):
            vt_ref[r, h, :head] = v_t[h * head : (h + 1) * head, r * n_k : (r + 1) * n_k]
            vt_ref[r, h, head:] = jnp.ones((tall - head, n_k), BF)


def project(core, own, other, wq, wk, wv_t, wg_t, n_heads, n_row=4):
    n_rows, n_q, ch = own.shape
    tall = ch // n_heads + 16
    row = lambda i: (i, 0, 0)
    fixed = pl.BlockSpec((ch, ch), lambda i: (0, 0))
    return pl.pallas_call(
        project_kernel,
        grid=(n_rows // n_row,),
        in_specs=[
            pl.BlockSpec(memory_space=pltpu.SMEM),
            pl.BlockSpec((n_row, n_q, ch), row),
            pl.BlockSpec((n_row, n_q, ch), row),
            fixed,
            fixed,
            fixed,
            fixed,
        ],
        out_specs=[
            pl.BlockSpec((n_row, n_q, ch), row),
            pl.BlockSpec((n_row, 2 * n_q, ch), row),
            pl.BlockSpec((n_row, n_heads, tall, 2 * n_q), lambda i: (i, 0, 0, 0)),
            pl.BlockSpec((n_row, ch, n_q), row),
        ],
        out_shape=[
            jax.ShapeDtypeStruct((n_rows, n_q, ch), BF),
            jax.ShapeDtypeStruct((n_rows, 2 * n_q, ch), BF),
            jax.ShapeDtypeStruct((n_rows, n_heads, tall, 2 * n_q), BF),
            jax.ShapeDtypeStruct((n_rows, ch, n_q), F32),
        ],
        name="project",
    )(core, own, other, wq, wk, wv_t, wg_t)


def attention_kernel(
    sub, q_ref, k_ref, vt_ref, gate_ref, two_ref, bias_ref, wo_ref, out_ref, raw_sc, bias_sc
):
    n_unit, n_k, _ = bias_sc.shape
    n_q, ch = q_ref.shape[1:]
    n_heads, tall, _ = vt_ref.shape[1:]
    head = ch // n_heads
    n_src, n_pay, _ = bias_ref.shape
    n_lt = n_q // LANES
    n_rh = n_src // 16
    n_col = n_q // sub // n_rh
    pairs = n_heads // 2

    @pl.when(pl.program_id(0) == 0)
    def _():
        def widen(d, carry):
            for v in range(4):
                at = pl.multiple_of((d * 4 + v) * n_pay, 8)
                for t in range(n_lt):
                    part = bias_ref[d * 4 + v, :, t * LANES : (t + 1) * LANES]
                    raw_sc[t, pl.ds(at, n_pay), :] = part.astype(F32) * -LOG2E
            return carry

        lax.fori_loop(0, n_src // 4, widen, 0)

        def turn(i, carry):
            s, h = i // n_heads, i % n_heads
            for u in range(n_lt):
                for t in range(n_lt):
                    rows = []
                    for r in range(16 * t, 16 * (t + 1)):
                        at = (r // sub * 2 + s) * n_col * n_pay + r % sub * n_heads + h
                        rows.append(raw_sc[u, pl.ds(at, n_col, stride=n_pay), :])
                    block = jnp.concatenate(rows, axis=0).T
                    at_k = pl.multiple_of(s * n_q + u * LANES, LANES)
                    at_q = pl.multiple_of(h % 2 * LANES, LANES)
                    bias_sc[t * pairs + h // 2, pl.ds(at_k, LANES), pl.ds(at_q, LANES)] = block
            return carry

        lax.fori_loop(0, 2 * n_heads, turn, 0)

    def row(r, carry):
        k = k_ref[r]
        lane_head = lax.broadcasted_iota(jnp.int32, (LANES, ch), 1) // head
        zero = jnp.zeros((), BF)

        def scores(n):
            t, hp = divmod(n, pairs)
            rows = q_ref[r, t * LANES : (t + 1) * LANES, :]
            both = [jnp.where(lane_head == 2 * hp + v, rows, zero) for v in range(2)]
            return dot_nt(k, jnp.concatenate(both, axis=0))

        s = scores(0)
        parts = []
        for n in range(n_unit):
            t, hp = divmod(n, pairs)
            ahead = scores(n + 1) if n + 1 < n_unit else None
            s = s - bias_sc[n]
            p = jnp.exp2(s - jnp.max(s, axis=0, keepdims=True)).astype(BF)
            both = vt_ref[r, 2 * hp : 2 * hp + 2].reshape(2 * tall, n_k)
            o = dot(both, p)
            for v in range(2):
                block = o[v * tall : (v + 1) * tall, v * LANES : (v + 1) * LANES]
                parts.append(block[:head] / block[head : head + 1])
            if hp == pairs - 1:
                cols = slice(t * LANES, (t + 1) * LANES)
                gated = (gate_ref[r, :, cols] * jnp.concatenate(parts, axis=0)).astype(BF)
                parts = []
                res = lax.dot_general(
                    gated, wo_ref[...], (((0,), (0,)), ((), ())), preferred_element_type=F32
                )
                out_ref[r, cols, :] = (two_ref[r, cols, :].astype(F32) + res).astype(BF)
            s = ahead
        return carry

    lax.fori_loop(0, q_ref.shape[0], row, 0, unroll=2)


def attention(q, k, vt, gate, two, bias, wo, sub, n_row=2):
    n_rows, n_q, ch = q.shape
    n_src, n_pay, _ = bias.shape
    n_heads = vt.shape[1]
    n_lt = n_q // LANES
    row = lambda i: (i, 0, 0)
    return pl.pallas_call(
        functools.partial(attention_kernel, sub),
        grid=(n_rows // n_row,),
        in_specs=[
            pl.BlockSpec((n_row, n_q, ch), row),
            pl.BlockSpec((n_row, 2 * n_q, ch), row),
            pl.BlockSpec((n_row,) + vt.shape[1:], lambda i: (i, 0, 0, 0)),
            pl.BlockSpec((n_row, ch, n_q), row),
            pl.BlockSpec((n_row, n_q, ch), row),
            pl.BlockSpec(bias.shape, lambda i: (0, 0, 0)),
            pl.BlockSpec(wo.shape, lambda i: (0, 0)),
        ],
        out_specs=pl.BlockSpec((n_row, n_q, ch), row),
        out_shape=jax.ShapeDtypeStruct(q.shape, BF),
        scratch_shapes=[
            pltpu.VMEM((n_lt, n_src * n_pay, LANES), F32),
            pltpu.VMEM((n_lt * n_heads // 2, 2 * n_q, 2 * LANES), F32),
        ],
        name="attention",
    )(q, k, vt, gate, two, bias, wo)


def body(
    pair_in,
    coords,
    chain_ids,
    coord_mask,
    gain_tri,
    gain_sum,
    gain_attn,
    w_tri_in,
    w_tri_out,
    w_bins,
    same_chain,
    w_query,
    w_attn,
    w_bias,
    w_attn_out,
):
    n_rh, n_core, n_col = (lax.axis_size(a) for a in ("rh", "core", "col"))
    rh, core, col = (lax.axis_index(a) for a in ("rh", "core", "col"))
    n_dev = n_rh * n_core * n_col
    every = ("rh", "core", "col")
    row_count, col_count, ch = pair_in.shape
    n_heads = w_bias.shape[1]
    n_bins = w_bins.shape[0]
    sub = row_count // n_col
    half = col_count // n_core
    n_pa = n_core * sub
    n_q = n_col * half

    to_move = (
        pair_in.reshape(sub, n_col, n_core, half, ch)
        .transpose(2, 1, 0, 3, 4)
        .reshape(n_core * n_col, sub, half, ch)
    )
    moved = exchange(to_move, ("core", "col"))
    moved = moved.reshape(n_core, n_col, sub, half, ch)

    packed = jnp.concatenate(
        [coords, chain_ids.astype(F32)[None], coord_mask.astype(F32)[None]], axis=0
    )
    packed = jnp.broadcast_to(packed, (n_rh * n_core, *packed.shape))
    known = exchange(packed, ("rh", "core"))
    known = known.reshape(n_rh, n_core, -1, row_count)
    near = lax.dynamic_index_in_dim(known, rh, 0, keepdims=False)
    near = near.transpose(1, 0, 2).reshape(-1, n_core, sub, n_col)
    near = lax.dynamic_index_in_dim(near, col, 3, keepdims=False).reshape(-1, n_pa)
    far = lax.dynamic_index_in_dim(known, core, 1, keepdims=False)
    far = far.transpose(1, 0, 2).reshape(-1, n_q)

    w_sides = w_tri_in[:, : 4 * ch].T
    sides = make_sides(pair_in, gain_tri, w_sides)
    sides = exchange(sides, every)
    product = triangle(sides, n_rh, n_core, n_col, row_count, col_count)
    back = exchange(product, every)
    two, normed, bias = update(
        back,
        moved,
        near,
        far,
        (gain_tri.reshape(1, ch), gain_sum.reshape(ch, 1), gain_attn.reshape(1, ch)),
        w_tri_in[:, 4 * ch :],
        w_tri_out,
        bin_weights(w_bins, same_chain),
        jnp.pad(w_bias.T, ((0, 16 - n_heads), (0, 0))),
        n_heads,
        n_bins,
    )

    n_pay = sub * n_heads
    spread = exchange(
        jnp.broadcast_to(
            bias.reshape(1, n_core, 1, n_pay, n_q), (n_rh, n_core, n_col, n_pay, n_q)
        ).reshape(n_dev, n_pay, n_q),
        every,
    )
    other = lax.ppermute(normed, every, [(d, d ^ n_col) for d in range(n_dev)])
    q, k, v_t, gate = project(
        core.reshape(1),
        normed,
        other,
        w_query,
        w_attn[:, :ch],
        w_attn[:, ch : 2 * ch].T,
        w_attn[:, 2 * ch :].T,
        n_heads,
    )
    result = attention(q, k, v_t, gate, two, spread, w_attn_out, sub)
    home = exchange(
        result.reshape(n_core, sub, n_col, half, ch)
        .transpose(0, 2, 1, 3, 4)
        .reshape(n_core * n_col, sub, half, ch),
        ("core", "col"),
    )
    return (
        home.reshape(n_core, n_col, sub, half, ch)
        .transpose(2, 1, 0, 3, 4)
        .reshape(row_count, col_count, ch)
    )


def solution(mesh):
    n_row, n_col = mesh.shape["row"], mesh.shape["col"]
    split = Mesh(mesh.devices.reshape(n_row // 2, 2, n_col), ("rh", "core", "col"))
    row = ("rh", "core")

    return jax.shard_map(
        body,
        mesh=split,
        in_specs=(P(row, "col", None), P(None, row), P(row), P(row)) + (P(),) * 11,
        out_specs=P(row, "col", None),
        check_vma=False,
    )
```

```python
import functools
import math

import jax
import jax.numpy as jnp
from jax import lax
from jax.experimental import pallas as pl
from jax.experimental.pallas import tpu as pltpu
from jax.sharding import Mesh
from jax.sharding import PartitionSpec as P

BF = jnp.bfloat16
F32 = jnp.float32
LOG2E = 1.4426950408889634
NT = (((1,), (1,)), ((), ()))
LANES = 128


def layer_norm(values, gain):
    center = values - jnp.mean(values, axis=-1, keepdims=True)
    spread = jnp.mean(center * center, axis=-1, keepdims=True)
    return center * lax.rsqrt(spread + 1e-05) * gain


def dot(a, b):
    return jnp.dot(a, b, preferred_element_type=F32)


def dot_nt(a, b):
    return lax.dot_general(a, b, NT, preferred_element_type=F32)


def exchange(x, axes):
    return lax.all_to_all(x, axes, split_axis=0, concat_axis=0, tiled=True)


def sides_kernel(col_ref, x_ref, gain_ref, w_ref, out_ref, *rest_refs):
    piece_refs, norm_sc, sc = rest_refs[:-2], rest_refs[-2], rest_refs[-1]
    n_rows, n_cols, ch = x_ref.shape
    n_col = len(piece_refs)
    for shift, piece_ref in enumerate(piece_refs):
        for a in range(n_rows // n_col):
            piece_ref[a] = x_ref[a * n_col + (col_ref[0] + shift) % n_col]
    n_out = out_ref.shape[1]
    third = n_rows // 3
    cut = LANES - n_cols

    def norm(i, carry):
        for u in range(4):
            norm_sc[i * 4 + u] = layer_norm(x_ref[i * 4 + u].astype(F32), gain_ref[...]).astype(BF)
        return carry

    lax.fori_loop(0, n_rows // 4, norm, 0, unroll=2)

    def sides(x):
        pr = dot_nt(w_ref[...], x)
        left = jax.nn.sigmoid(pr[:ch]) * pr[ch : 2 * ch]
        right = jax.nn.sigmoid(pr[2 * ch : 3 * ch]) * pr[3 * ch :]
        return left, right

    def put(row, value):
        sc[pl.ds(row, ch, stride=n_out), :] = value

    def main(s, carry):
        x = jnp.concatenate(
            [
                norm_sc[s],
                norm_sc[third + s, :cut],
                norm_sc[2 * third + s],
                norm_sc[third + s, cut : 2 * cut],
            ],
            axis=0,
        )
        left, right = sides(x)
        put(s, left[:, :LANES])
        put(third + s, left[:, LANES:])
        put(2 * third + s, right[:, :LANES])
        put(3 * third + s, right[:, LANES:])
        return carry

    lax.fori_loop(0, third, main, 0, unroll=4)

    is_left = lax.broadcasted_iota(jnp.int32, (ch, LANES), 1) < LANES // 2

    def rest(s, carry):
        one = norm_sc[third + s, 2 * cut :]
        two = norm_sc[third + third // 2 + s, 2 * cut :]
        left, right = sides(jnp.concatenate([one, two, one, two], axis=0))
        put(4 * third + s, jnp.where(is_left, left, right))
        return carry

    lax.fori_loop(0, third // 2, rest, 0, unroll=4)

    def emit(c, carry):
        out_ref[c] = sc[pl.ds(pl.multiple_of(c * n_out, 8), n_out), :].astype(BF)
        return carry

    lax.fori_loop(0, ch, emit, 0, unroll=16)


def make_sides(col, pair, gain, w_t, n_col):
    n_rows, n_cols, ch = pair.shape
    n_out = 2 * n_rows * n_cols // LANES
    piece = jax.ShapeDtypeStruct((n_rows // n_col, n_cols, ch), BF)
    return pl.pallas_call(
        sides_kernel,
        in_specs=[pl.BlockSpec(memory_space=pltpu.SMEM)] + [pl.BlockSpec()] * 3,
        out_shape=[jax.ShapeDtypeStruct((ch, n_out, LANES), BF)] + [piece] * n_col,
        scratch_shapes=[
            pltpu.VMEM(pair.shape, BF),
            pltpu.VMEM((ch * n_out, LANES), F32),
        ],
        name="sides",
    )(col, pair, gain.reshape(1, ch), w_t)


def triangle_kernel(n_rh, n_core, n_col, n_rows, n_cols, in_ref, out_ref, l_sc, r_sc, p_sc):
    third = n_rows // 3
    cut = LANES - n_cols
    total = n_rh * n_core * n_rows
    n_pa = n_core * n_rows // n_col
    n_lt = total // n_core // LANES
    lane = lax.broadcasted_iota(jnp.int32, (third, LANES), 1)

    def middle(a, b, c):
        return jnp.where(
            lane < cut,
            pltpu.roll(a, cut, 1),
            jnp.where(lane < 2 * cut, pltpu.roll(b, 2 * cut, 1), jnp.where(lane < n_cols, c, 0.0)),
        )

    def unpack(rh, carry):
        for p in range(n_core):
            for c in range(n_col):
                blk = in_ref[(rh * n_core + p) * n_col + c].astype(F32)
                b = [blk[third * t : third * (t + 1)] for t in range(4)]
                last = blk[4 * third :]
                keep = [jnp.where(lane < n_cols, t, 0.0) for t in b]
                lc = jnp.concatenate([pltpu.roll(last, 2 * cut, 1), pltpu.roll(last, cut, 1)], axis=0)
                rc = jnp.concatenate([last, pltpu.roll(last, 3 * cut, 1)], axis=0)
                left = jnp.concatenate([keep[0], middle(b[0], b[1], lc), keep[1]], axis=0)
                right = jnp.concatenate([keep[2], middle(b[2], b[3], rc), keep[3]], axis=0)
                lanes = slice(c * LANES, (c + 1) * LANES)
                at_l = pl.multiple_of((rh * n_core + p) * n_rows, 16)
                at_r = pl.multiple_of((p * n_rh + rh) * n_rows, 16)
                l_sc[pl.ds(at_l, n_rows), lanes] = left.astype(BF)
                r_sc[pl.ds(at_r, n_rows), lanes] = right.astype(BF)
        return carry

    lax.fori_loop(0, n_rh, unpack, 0)
    wide = 2 * LANES
    for t in range(total // wide):
        part = dot_nt(l_sc[...], r_sc[t * wide : (t + 1) * wide, :])
        p_sc[2 * t] = part[:, :LANES]
        p_sc[2 * t + 1] = part[:, LANES:]

    def pack(rh, carry):
        for core in range(n_core):
            for c in range(n_col):
                rows = pl.ds(rh * n_core * n_rows + c, n_pa, stride=n_col)
                parts = [p_sc[core * n_lt + t, rows, :] for t in range(n_lt)]
                out_ref[(rh * n_core + core) * n_col + c] = jnp.concatenate(parts, axis=0).astype(BF)
        return carry

    lax.fori_loop(0, n_rh, pack, 0)


def triangle(sides, n_rh, n_core, n_col, n_rows, n_cols):
    total = n_rh * n_core * n_rows
    n_pa = n_core * n_rows // n_col
    n_lt = total // n_core // LANES
    return pl.pallas_call(
        functools.partial(triangle_kernel, n_rh, n_core, n_col, n_rows, n_cols),
        out_shape=jax.ShapeDtypeStruct((sides.shape[0], n_lt * n_pa, LANES), BF),
        scratch_shapes=[
            pltpu.VMEM((total, n_col * LANES), BF),
            pltpu.VMEM((total, n_col * LANES), BF),
            pltpu.VMEM((total // LANES, total, LANES), F32),
        ],
        name="triangle",
    )(sides)


def unit_norm(x, ones):
    center = x.astype(F32) - dot(x, ones[: x.shape[1]])
    square = center * center
    high = square.astype(BF)
    low = (square - high.astype(F32)).astype(BF)
    spread = dot(jnp.concatenate([high, low], axis=1), ones)
    return center * lax.rsqrt(spread + 1e-05)


def update_kernel(
    n_bins,
    place_ref,
    back_ref,
    keep_ref,
    other_ref,
    near_ref,
    far_ref,
    gain_tri_ref,
    gain_sum_ref,
    gain_attn_ref,
    wgo_ref,
    wout_ref,
    wbins_ref,
    wbias_ref,
    two_ref,
    normed_ref,
    bias_ref,
    sc,
):
    ch, n_in, _ = back_ref.shape
    n_q = far_ref.shape[1]
    n_lt = n_q // LANES
    n_pa = n_in // n_lt
    n_in8 = sc.shape[0] // ch
    n_col = keep_ref.shape[0]
    n_heads = bias_ref.shape[1]
    tn = (((0,), (0,)), ((), ()))

    @pl.when(pl.program_id(0) == 0)
    def _():
        def widen(c, carry):
            sc[pl.ds(pl.multiple_of(c * n_in8, 8), n_in), :] = back_ref[c].astype(F32)
            return carry

        lax.fori_loop(0, ch, widen, 0, unroll=16)

    ones = jnp.full((2 * ch, ch), 1.0 / ch, BF)
    n_row = two_ref.shape[0]
    n_feat = wbins_ref.shape[0] // 3
    bin_at = lax.broadcasted_iota(jnp.int32, (n_feat, 1), 0)
    centres = 2.0 + 20.0 * bin_at.astype(F32) / (n_bins - 1)
    parts = []
    pairs = []
    feats = []
    for v in range(n_row):
        pa = pl.program_id(0) * n_row + v
        for t in range(n_lt):
            x = sc[pl.ds(t * n_pa + pa, ch, stride=n_in8), :]
            center = x - jnp.mean(x, axis=0, keepdims=True)
            spread = jnp.mean(center * center, axis=0, keepdims=True)
            parts.append((center * lax.rsqrt(spread + 1e-05) * gain_sum_ref[...]).astype(BF))
        mine = place_ref[0] == pl.program_id(0) * n_row // (n_pa // 2)
        for c in range(n_col):
            shift = (place_ref[1] + n_col - c) % n_col
            pairs.append(jnp.where(mine, keep_ref[shift, v], other_ref[shift, v]))
        square = jnp.zeros((1, n_q), F32)
        for f in range(3):
            off = far_ref[f : f + 1, :] - near_ref[f, pa]
            square = square + off * off
        shared = (far_ref[3:4, :] == near_ref[3, pa]).astype(F32)
        mask = far_ref[4:5, :] * near_ref[4, pa]
        z = (jnp.sqrt(square + 1.0) - centres) * ((n_bins - 1) / 25.0)
        bins = jnp.exp(-(z * z)) * mask
        feats.append(jnp.where(bin_at < n_bins, bins, jnp.where(bin_at == n_bins, shared, 0.0)))
    tri = lax.dot_general(
        jnp.concatenate(parts, axis=1), wout_ref[...], tn, preferred_element_type=F32
    )
    pair = jnp.concatenate(pairs, axis=0)
    normed_pair = (unit_norm(pair, ones) * gain_tri_ref[...]).astype(BF)
    gate = jax.nn.sigmoid(dot(normed_pair, wgo_ref[...]))
    feats = jnp.concatenate(feats, axis=1)
    high = feats.astype(BF)
    low = (feats - high.astype(F32)).astype(BF)
    binned = lax.dot_general(
        jnp.concatenate([high, low, high], axis=0), wbins_ref[...], tn, preferred_element_type=F32
    )
    two = (pair.astype(F32) + gate * tri + binned).astype(BF)
    normed = (unit_norm(two, ones) * gain_attn_ref[...]).astype(BF)
    bias = dot_nt(wbias_ref[...], normed)[:n_heads].astype(BF)
    for v in range(n_row):
        two_ref[v] = two[v * n_q : (v + 1) * n_q]
        normed_ref[v] = normed[v * n_q : (v + 1) * n_q]
        bias_ref[v] = bias[:, v * n_q : (v + 1) * n_q]


def bin_weights(w_bins, same_chain):
    n_feat = -(-(w_bins.shape[0] + 1) // 16) * 16
    rows = jnp.concatenate([w_bins, same_chain[None]], axis=0)
    rows = jnp.pad(rows, ((0, n_feat - rows.shape[0]), (0, 0)))
    high = lax.reduce_precision(rows, 8, 7)
    return jnp.concatenate([high, high, rows - high], axis=0).astype(BF)


def update(place, back, keep, other, near, far, gains, wgo, wout, wbins, wbias_t, n_heads, n_bins, n_row=6):
    ch, n_in, _ = back.shape
    n_col, sub, half, _ = keep.shape
    n_q = n_col * half
    n_pa = 2 * sub
    n_in8 = -(-n_in // 8) * 8
    per = sub // n_row
    fixed = lambda i: (0, 0)
    row = lambda i: (i, 0, 0)
    return pl.pallas_call(
        functools.partial(update_kernel, n_bins),
        grid=(n_pa // n_row,),
        in_specs=[
            pl.BlockSpec(memory_space=pltpu.SMEM),
            pl.BlockSpec(back.shape, lambda i: (0, 0, 0)),
            pl.BlockSpec((n_col, n_row, half, ch), lambda i: (0, i % per, 0, 0)),
            pl.BlockSpec((n_col, n_row, half, ch), lambda i: (0, i % per, 0, 0)),
            pl.BlockSpec(memory_space=pltpu.SMEM),
            pl.BlockSpec(far.shape, fixed),
            pl.BlockSpec((1, ch), fixed),
            pl.BlockSpec((ch, 1), fixed),
            pl.BlockSpec((1, ch), fixed),
            pl.BlockSpec(wgo.shape, fixed),
            pl.BlockSpec(wout.shape, fixed),
            pl.BlockSpec(wbins.shape, fixed),
            pl.BlockSpec(wbias_t.shape, fixed),
        ],
        out_specs=[
            pl.BlockSpec((n_row, n_q, ch), row),
            pl.BlockSpec((n_row, n_q, ch), row),
            pl.BlockSpec((n_row, n_heads, n_q), row),
        ],
        out_shape=[
            jax.ShapeDtypeStruct((n_pa, n_q, ch), BF),
            jax.ShapeDtypeStruct((n_pa, n_q, ch), BF),
            jax.ShapeDtypeStruct((n_pa, n_heads, n_q), BF),
        ],
        scratch_shapes=[pltpu.VMEM((ch * n_in8, LANES), F32)],
        name="update",
    )(place, back, keep, other, near, far, gains[0], gains[1], gains[2], wgo, wout, wbins, wbias_t)


def project_kernel(
    core_ref, own_ref, other_ref, wq_ref, wk_ref, wv_ref, wg_ref, q_ref, k_ref, vt_ref, gate_ref
):
    n_heads, tall, n_k = vt_ref.shape[1:]
    head = wv_ref.shape[0] // n_heads
    first = core_ref[0] == 0
    n_row, n_q, ch = own_ref.shape
    own, other = own_ref[...], other_ref[...]
    full = jnp.concatenate(
        [jnp.where(first, own, other), jnp.where(first, other, own)], axis=1
    ).reshape(n_row * n_k, ch)
    own = own.reshape(n_row * n_q, ch)
    scale = LOG2E / math.sqrt(head)
    q_ref[...] = (dot(own, wq_ref[...]) * scale).astype(BF).reshape(n_row, n_q, ch)
    gate = jax.nn.sigmoid(dot_nt(wg_ref[...], own))
    k_ref[...] = dot(full, wk_ref[...]).astype(BF).reshape(n_row, n_k, ch)
    v_t = dot_nt(wv_ref[...], full).astype(BF)
    for r in range(n_row):
        gate_ref[r] = gate[:, r * n_q : (r + 1) * n_q]
        for h in range(n_heads):
            vt_ref[r, h, :head] = v_t[h * head : (h + 1) * head, r * n_k : (r + 1) * n_k]
            vt_ref[r, h, head:] = jnp.ones((tall - head, n_k), BF)


def project(core, own, other, wq, wk, wv_t, wg_t, n_heads, n_row=4):
    n_rows, n_q, ch = own.shape
    tall = ch // n_heads + 16
    row = lambda i: (i, 0, 0)
    fixed = pl.BlockSpec((ch, ch), lambda i: (0, 0))
    return pl.pallas_call(
        project_kernel,
        grid=(n_rows // n_row,),
        in_specs=[
            pl.BlockSpec(memory_space=pltpu.SMEM),
            pl.BlockSpec((n_row, n_q, ch), row),
            pl.BlockSpec((n_row, n_q, ch), row),
            fixed,
            fixed,
            fixed,
            fixed,
        ],
        out_specs=[
            pl.BlockSpec((n_row, n_q, ch), row),
            pl.BlockSpec((n_row, 2 * n_q, ch), row),
            pl.BlockSpec((n_row, n_heads, tall, 2 * n_q), lambda i: (i, 0, 0, 0)),
            pl.BlockSpec((n_row, ch, n_q), row),
        ],
        out_shape=[
            jax.ShapeDtypeStruct((n_rows, n_q, ch), BF),
            jax.ShapeDtypeStruct((n_rows, 2 * n_q, ch), BF),
            jax.ShapeDtypeStruct((n_rows, n_heads, tall, 2 * n_q), BF),
            jax.ShapeDtypeStruct((n_rows, ch, n_q), F32),
        ],
        name="project",
    )(core, own, other, wq, wk, wv_t, wg_t)


def attention_kernel(
    sub, q_ref, k_ref, vt_ref, gate_ref, two_ref, bias_ref, wo_ref, out_ref, raw_sc, bias_sc
):
    n_unit, n_k, _ = bias_sc.shape
    n_q, ch = q_ref.shape[1:]
    n_heads, tall, _ = vt_ref.shape[1:]
    head = ch // n_heads
    n_src, n_pay, _ = bias_ref.shape
    n_lt = n_q // LANES
    n_rh = n_src // 16
    n_col = n_q // sub // n_rh
    pairs = n_heads // 2

    @pl.when(pl.program_id(0) == 0)
    def _():
        def widen(d, carry):
            for v in range(4):
                at = pl.multiple_of((d * 4 + v) * n_pay, 8)
                for t in range(n_lt):
                    part = bias_ref[d * 4 + v, :, t * LANES : (t + 1) * LANES]
                    raw_sc[t, pl.ds(at, n_pay), :] = part.astype(F32) * -LOG2E
            return carry

        lax.fori_loop(0, n_src // 4, widen, 0)

        def turn(i, carry):
            s, h = i // n_heads, i % n_heads
            for u in range(n_lt):
                for t in range(n_lt):
                    rows = []
                    for r in range(16 * t, 16 * (t + 1)):
                        at = (r // sub * 2 + s) * n_col * n_pay + r % sub * n_heads + h
                        rows.append(raw_sc[u, pl.ds(at, n_col, stride=n_pay), :])
                    block = jnp.concatenate(rows, axis=0).T
                    at_k = pl.multiple_of(s * n_q + u * LANES, LANES)
                    at_q = pl.multiple_of(h % 2 * LANES, LANES)
                    bias_sc[t * pairs + h // 2, pl.ds(at_k, LANES), pl.ds(at_q, LANES)] = block
            return carry

        lax.fori_loop(0, 2 * n_heads, turn, 0)

    def row(r, carry):
        k = k_ref[r]
        lane_head = lax.broadcasted_iota(jnp.int32, (LANES, ch), 1) // head
        zero = jnp.zeros((), BF)

        def scores(n):
            t, hp = divmod(n, pairs)
            rows = q_ref[r, t * LANES : (t + 1) * LANES, :]
            both = [jnp.where(lane_head == 2 * hp + v, rows, zero) for v in range(2)]
            return dot_nt(k, jnp.concatenate(both, axis=0))

        s = scores(0)
        parts = []
        for n in range(n_unit):
            t, hp = divmod(n, pairs)
            ahead = scores(n + 1) if n + 1 < n_unit else None
            s = s - bias_sc[n]
            p = jnp.exp2(s - jnp.max(s, axis=0, keepdims=True)).astype(BF)
            both = vt_ref[r, 2 * hp : 2 * hp + 2].reshape(2 * tall, n_k)
            o = dot(both, p)
            for v in range(2):
                block = o[v * tall : (v + 1) * tall, v * LANES : (v + 1) * LANES]
                parts.append(block[:head] / block[head : head + 1])
            if hp == pairs - 1:
                cols = slice(t * LANES, (t + 1) * LANES)
                gated = (gate_ref[r, :, cols] * jnp.concatenate(parts, axis=0)).astype(BF)
                parts = []
                res = lax.dot_general(
                    gated, wo_ref[...], (((0,), (0,)), ((), ())), preferred_element_type=F32
                )
                out_ref[r, cols, :] = (two_ref[r, cols, :].astype(F32) + res).astype(BF)
            s = ahead
        return carry

    lax.fori_loop(0, q_ref.shape[0], row, 0, unroll=2)


def attention(q, k, vt, gate, two, bias, wo, sub, n_row=2):
    n_rows, n_q, ch = q.shape
    n_src, n_pay, _ = bias.shape
    n_heads = vt.shape[1]
    n_lt = n_q // LANES
    row = lambda i: (i, 0, 0)
    return pl.pallas_call(
        functools.partial(attention_kernel, sub),
        grid=(n_rows // n_row,),
        in_specs=[
            pl.BlockSpec((n_row, n_q, ch), row),
            pl.BlockSpec((n_row, 2 * n_q, ch), row),
            pl.BlockSpec((n_row,) + vt.shape[1:], lambda i: (i, 0, 0, 0)),
            pl.BlockSpec((n_row, ch, n_q), row),
            pl.BlockSpec((n_row, n_q, ch), row),
            pl.BlockSpec(bias.shape, lambda i: (0, 0, 0)),
            pl.BlockSpec(wo.shape, lambda i: (0, 0)),
        ],
        out_specs=pl.BlockSpec((n_row, n_q, ch), row),
        out_shape=jax.ShapeDtypeStruct(q.shape, BF),
        scratch_shapes=[
            pltpu.VMEM((n_lt, n_src * n_pay, LANES), F32),
            pltpu.VMEM((n_lt * n_heads // 2, 2 * n_q, 2 * LANES), F32),
        ],
        name="attention",
    )(q, k, vt, gate, two, bias, wo)


def body(
    pair_in,
    coords,
    chain_ids,
    coord_mask,
    gain_tri,
    gain_sum,
    gain_attn,
    w_tri_in,
    w_tri_out,
    w_bins,
    same_chain,
    w_query,
    w_attn,
    w_bias,
    w_attn_out,
):
    n_rh, n_core, n_col = (lax.axis_size(a) for a in ("rh", "core", "col"))
    rh, core, col = (lax.axis_index(a) for a in ("rh", "core", "col"))
    n_dev = n_rh * n_core * n_col
    every = ("rh", "core", "col")
    row_count, col_count, ch = pair_in.shape
    n_heads = w_bias.shape[1]
    n_bins = w_bins.shape[0]
    sub = row_count // n_col
    half = col_count // n_core
    n_pa = n_core * sub
    n_q = n_col * half

    w_sides = w_tri_in[:, : 4 * ch].T
    sides, *pieces = make_sides(col.reshape(1), pair_in, gain_tri, w_sides, n_col)
    sides = exchange(sides, every)

    pieces = [pieces[0]] + [
        lax.ppermute(pieces[d], "col", [(i, (i + d) % n_col) for i in range(n_col)])
        for d in range(1, n_col)
    ]
    whole = jnp.stack(pieces).reshape(n_col, sub, n_core, half, ch)
    keep = lax.dynamic_index_in_dim(whole, core, 2, keepdims=False)
    give = lax.dynamic_index_in_dim(whole, 1 - core, 2, keepdims=False)
    other_pair = lax.ppermute(give, "core", [(0, 1), (1, 0)])

    packed = jnp.concatenate(
        [coords, chain_ids.astype(F32)[None], coord_mask.astype(F32)[None]], axis=0
    ).reshape(1, -1)
    n_row = n_rh * n_core
    step = 1
    while step < n_row:
        swap = [(r, r ^ step) for r in range(n_row)]
        packed = jnp.concatenate([packed, lax.ppermute(packed, ("rh", "core"), swap)], axis=0)
        step *= 2
    at = jnp.arange(n_row) ^ (rh * n_core + core)
    known = packed[at].reshape(n_rh, n_core, -1, row_count)
    near = lax.dynamic_index_in_dim(known, rh, 0, keepdims=False)
    near = near.transpose(1, 0, 2).reshape(-1, n_core, sub, n_col)
    near = lax.dynamic_index_in_dim(near, col, 3, keepdims=False).reshape(-1, n_pa)
    far = lax.dynamic_index_in_dim(known, core, 1, keepdims=False)
    far = far.transpose(1, 0, 2).reshape(-1, n_q)

    product = triangle(sides, n_rh, n_core, n_col, row_count, col_count)
    back = exchange(product, every)
    two, normed, bias = update(
        jnp.stack([core, col]),
        back,
        keep,
        other_pair,
        near,
        far,
        (gain_tri.reshape(1, ch), gain_sum.reshape(ch, 1), gain_attn.reshape(1, ch)),
        w_tri_in[:, 4 * ch :],
        w_tri_out,
        bin_weights(w_bins, same_chain),
        jnp.pad(w_bias.T, ((0, 16 - n_heads), (0, 0))),
        n_heads,
        n_bins,
    )

    n_pay = sub * n_heads
    spread = exchange(
        jnp.broadcast_to(
            bias.reshape(1, n_core, 1, n_pay, n_q), (n_rh, n_core, n_col, n_pay, n_q)
        ).reshape(n_dev, n_pay, n_q),
        every,
    )
    other = lax.ppermute(normed, every, [(d, d ^ n_col) for d in range(n_dev)])
    q, k, v_t, gate = project(
        core.reshape(1),
        normed,
        other,
        w_query,
        w_attn[:, :ch],
        w_attn[:, ch : 2 * ch].T,
        w_attn[:, 2 * ch :].T,
        n_heads,
    )
    result = attention(q, k, v_t, gate, two, spread, w_attn_out, sub)
    home = exchange(
        result.reshape(n_core, sub, n_col, half, ch)
        .transpose(0, 2, 1, 3, 4)
        .reshape(n_core * n_col, sub, half, ch),
        ("core", "col"),
    )
    return (
        home.reshape(n_core, n_col, sub, half, ch)
        .transpose(2, 1, 0, 3, 4)
        .reshape(row_count, col_count, ch)
    )


def solution(mesh):
    n_row, n_col = mesh.shape["row"], mesh.shape["col"]
    split = Mesh(mesh.devices.reshape(n_row // 2, 2, n_col), ("rh", "core", "col"))
    row = ("rh", "core")

    return jax.shard_map(
        body,
        mesh=split,
        in_specs=(P(row, "col", None), P(None, row), P(row), P(row)) + (P(),) * 11,
        out_specs=P(row, "col", None),
        check_vma=False,
    )
```

```python
import functools
import math

import jax
import jax.numpy as jnp
from jax import lax
from jax.experimental import pallas as pl
from jax.experimental.pallas import tpu as pltpu
from jax.sharding import Mesh
from jax.sharding import PartitionSpec as P

BF = jnp.bfloat16
F32 = jnp.float32
LOG2E = 1.4426950408889634
NT = (((1,), (1,)), ((), ()))
LANES = 128


def layer_norm(values, gain):
    center = values - jnp.mean(values, axis=-1, keepdims=True)
    spread = jnp.mean(center * center, axis=-1, keepdims=True)
    return center * lax.rsqrt(spread + 1e-05) * gain


def dot(a, b):
    return jnp.dot(a, b, preferred_element_type=F32)


def dot_nt(a, b):
    return lax.dot_general(a, b, NT, preferred_element_type=F32)


def exchange(x, axes):
    return lax.all_to_all(x, axes, split_axis=0, concat_axis=0, tiled=True)


def sides_kernel(col_ref, x_ref, gain_ref, w_ref, out_ref, *rest_refs):
    piece_refs, norm_sc, sc = rest_refs[:-2], rest_refs[-2], rest_refs[-1]
    n_rows, n_cols, ch = x_ref.shape
    n_col = len(piece_refs)
    for shift, piece_ref in enumerate(piece_refs):
        for a in range(n_rows // n_col):
            piece_ref[a] = x_ref[a * n_col + (col_ref[0] + shift) % n_col]
    n_out = out_ref.shape[1]
    third = n_rows // 3
    cut = LANES - n_cols

    def norm(i, carry):
        for u in range(4):
            norm_sc[i * 4 + u] = layer_norm(x_ref[i * 4 + u].astype(F32), gain_ref[...]).astype(BF)
        return carry

    lax.fori_loop(0, n_rows // 4, norm, 0, unroll=2)

    def sides(x):
        pr = dot_nt(w_ref[...], x)
        left = jax.nn.sigmoid(pr[:ch]) * pr[ch : 2 * ch]
        right = jax.nn.sigmoid(pr[2 * ch : 3 * ch]) * pr[3 * ch :]
        return left, right

    def put(row, value):
        sc[pl.ds(row, ch, stride=n_out), :] = value

    def main(s, carry):
        x = jnp.concatenate(
            [
                norm_sc[s],
                norm_sc[third + s, :cut],
                norm_sc[2 * third + s],
                norm_sc[third + s, cut : 2 * cut],
            ],
            axis=0,
        )
        left, right = sides(x)
        put(s, left[:, :LANES])
        put(third + s, left[:, LANES:])
        put(2 * third + s, right[:, :LANES])
        put(3 * third + s, right[:, LANES:])
        return carry

    lax.fori_loop(0, third, main, 0, unroll=4)

    is_left = lax.broadcasted_iota(jnp.int32, (ch, LANES), 1) < LANES // 2

    def rest(s, carry):
        one = norm_sc[third + s, 2 * cut :]
        two = norm_sc[third + third // 2 + s, 2 * cut :]
        left, right = sides(jnp.concatenate([one, two, one, two], axis=0))
        put(4 * third + s, jnp.where(is_left, left, right))
        return carry

    lax.fori_loop(0, third // 2, rest, 0, unroll=4)

    def emit(c, carry):
        out_ref[c] = sc[pl.ds(pl.multiple_of(c * n_out, 8), n_out), :].astype(BF)
        return carry

    lax.fori_loop(0, ch, emit, 0, unroll=16)


def make_sides(col, pair, gain, w_t, n_col):
    n_rows, n_cols, ch = pair.shape
    n_out = 2 * n_rows * n_cols // LANES
    piece = jax.ShapeDtypeStruct((n_rows // n_col, n_cols, ch), BF)
    return pl.pallas_call(
        sides_kernel,
        in_specs=[pl.BlockSpec(memory_space=pltpu.SMEM)] + [pl.BlockSpec()] * 3,
        out_shape=[jax.ShapeDtypeStruct((ch, n_out, LANES), BF)] + [piece] * n_col,
        scratch_shapes=[
            pltpu.VMEM(pair.shape, BF),
            pltpu.VMEM((ch * n_out, LANES), F32),
        ],
        name="sides",
    )(col, pair, gain.reshape(1, ch), w_t)


def triangle_kernel(n_rh, n_core, n_col, n_rows, n_cols, in_ref, out_ref, l_sc, r_sc, p_sc):
    third = n_rows // 3
    cut = LANES - n_cols
    total = n_rh * n_core * n_rows
    n_pa = n_core * n_rows // n_col
    n_lt = total // n_core // LANES
    lane = lax.broadcasted_iota(jnp.int32, (third, LANES), 1)

    def middle(a, b, c):
        return jnp.where(
            lane < cut,
            pltpu.roll(a, cut, 1),
            jnp.where(lane < 2 * cut, pltpu.roll(b, 2 * cut, 1), jnp.where(lane < n_cols, c, 0.0)),
        )

    def unpack(rh, carry):
        for p in range(n_core):
            for c in range(n_col):
                blk = in_ref[(rh * n_core + p) * n_col + c].astype(F32)
                b = [blk[third * t : third * (t + 1)] for t in range(4)]
                last = blk[4 * third :]
                keep = [jnp.where(lane < n_cols, t, 0.0) for t in b]
                lc = jnp.concatenate([pltpu.roll(last, 2 * cut, 1), pltpu.roll(last, cut, 1)], axis=0)
                rc = jnp.concatenate([last, pltpu.roll(last, 3 * cut, 1)], axis=0)
                left = jnp.concatenate([keep[0], middle(b[0], b[1], lc), keep[1]], axis=0)
                right = jnp.concatenate([keep[2], middle(b[2], b[3], rc), keep[3]], axis=0)
                lanes = slice(c * LANES, (c + 1) * LANES)
                at_l = pl.multiple_of((rh * n_core + p) * n_rows, 16)
                at_r = pl.multiple_of((p * n_rh + rh) * n_rows, 16)
                l_sc[pl.ds(at_l, n_rows), lanes] = left.astype(BF)
                r_sc[pl.ds(at_r, n_rows), lanes] = right.astype(BF)
        return carry

    lax.fori_loop(0, n_rh, unpack, 0)
    wide = 2 * LANES
    for t in range(total // wide):
        part = dot_nt(l_sc[...], r_sc[t * wide : (t + 1) * wide, :])
        p_sc[2 * t] = part[:, :LANES]
        p_sc[2 * t + 1] = part[:, LANES:]

    def pack(rh, carry):
        for core in range(n_core):
            for c in range(n_col):
                rows = pl.ds(rh * n_core * n_rows + c, n_pa, stride=n_col)
                parts = [p_sc[core * n_lt + t, rows, :] for t in range(n_lt)]
                out_ref[(rh * n_core + core) * n_col + c] = jnp.concatenate(parts, axis=0).astype(BF)
        return carry

    lax.fori_loop(0, n_rh, pack, 0)


def triangle(sides, n_rh, n_core, n_col, n_rows, n_cols):
    total = n_rh * n_core * n_rows
    n_pa = n_core * n_rows // n_col
    n_lt = total // n_core // LANES
    return pl.pallas_call(
        functools.partial(triangle_kernel, n_rh, n_core, n_col, n_rows, n_cols),
        out_shape=jax.ShapeDtypeStruct((sides.shape[0], n_lt * n_pa, LANES), BF),
        scratch_shapes=[
            pltpu.VMEM((total, n_col * LANES), BF),
            pltpu.VMEM((total, n_col * LANES), BF),
            pltpu.VMEM((total // LANES, total, LANES), F32),
        ],
        compiler_params=pltpu.CompilerParams(vmem_limit_bytes=24 << 20),
        name="triangle",
    )(sides)


def unit_norm(x, ones):
    center = x.astype(F32) - dot(x, ones[: x.shape[1]])
    square = center * center
    high = square.astype(BF)
    low = (square - high.astype(F32)).astype(BF)
    spread = dot(jnp.concatenate([high, low], axis=1), ones)
    return center * lax.rsqrt(spread + 1e-05)


def update_kernel(
    n_bins,
    place_ref,
    back_ref,
    keep_ref,
    other_ref,
    near_ref,
    far_ref,
    gain_tri_ref,
    gain_sum_ref,
    gain_attn_ref,
    wgo_ref,
    wout_ref,
    wbins_ref,
    wbias_ref,
    two_ref,
    normed_ref,
    bias_ref,
    sc,
):
    ch, n_in, _ = back_ref.shape
    n_q = far_ref.shape[1]
    n_lt = n_q // LANES
    n_pa = n_in // n_lt
    n_in8 = sc.shape[0] // ch
    n_col = keep_ref.shape[0]
    n_heads = bias_ref.shape[3] // two_ref.shape[0]
    tn = (((0,), (0,)), ((), ()))

    @pl.when(pl.program_id(0) == 0)
    def _():
        def widen(c, carry):
            sc[pl.ds(pl.multiple_of(c * n_in8, 8), n_in), :] = back_ref[c].astype(F32)
            return carry

        lax.fori_loop(0, ch, widen, 0, unroll=16)

    ones = jnp.full((2 * ch, ch), 1.0 / ch, BF)
    n_row = two_ref.shape[0]
    n_feat = wbins_ref.shape[0] // 3
    bin_at = lax.broadcasted_iota(jnp.int32, (n_feat, 1), 0)
    centres = 2.0 + 20.0 * bin_at.astype(F32) / (n_bins - 1)
    parts = []
    pairs = []
    feats = []
    for v in range(n_row):
        pa = pl.program_id(0) * n_row + v
        for t in range(n_lt):
            x = sc[pl.ds(t * n_pa + pa, ch, stride=n_in8), :]
            center = x - jnp.mean(x, axis=0, keepdims=True)
            spread = jnp.mean(center * center, axis=0, keepdims=True)
            parts.append((center * lax.rsqrt(spread + 1e-05) * gain_sum_ref[...]).astype(BF))
        mine = place_ref[0] == pl.program_id(0) * n_row // (n_pa // 2)
        for c in range(n_col):
            shift = (place_ref[1] + n_col - c) % n_col
            pairs.append(jnp.where(mine, keep_ref[shift, v], other_ref[shift, v]))
        square = jnp.zeros((1, n_q), F32)
        for f in range(3):
            off = far_ref[f : f + 1, :] - near_ref[f, pa]
            square = square + off * off
        shared = (far_ref[3:4, :] == near_ref[3, pa]).astype(F32)
        mask = far_ref[4:5, :] * near_ref[4, pa]
        z = (jnp.sqrt(square + 1.0) - centres) * ((n_bins - 1) / 25.0)
        bins = jnp.exp(-(z * z)) * mask
        feats.append(jnp.where(bin_at < n_bins, bins, jnp.where(bin_at == n_bins, shared, 0.0)))
    tri = lax.dot_general(
        jnp.concatenate(parts, axis=1), wout_ref[...], tn, preferred_element_type=F32
    )
    pair = jnp.concatenate(pairs, axis=0)
    normed_pair = (unit_norm(pair, ones) * gain_tri_ref[...]).astype(BF)
    gate = jax.nn.sigmoid(dot(normed_pair, wgo_ref[...]))
    feats = jnp.concatenate(feats, axis=1)
    high = feats.astype(BF)
    low = (feats - high.astype(F32)).astype(BF)
    binned = lax.dot_general(
        jnp.concatenate([high, low, high], axis=0), wbins_ref[...], tn, preferred_element_type=F32
    )
    two = (pair.astype(F32) + gate * tri + binned).astype(BF)
    normed = (unit_norm(two, ones) * gain_attn_ref[...]).astype(BF)
    bias = dot_nt(wbias_ref[...], normed)[:n_heads]
    for v in range(n_row):
        two_ref[v] = two[v * n_q : (v + 1) * n_q]
        normed_ref[v] = normed[v * n_q : (v + 1) * n_q]
    bias = jnp.concatenate([bias[:, v * n_q : (v + 1) * n_q] for v in range(n_row)], axis=0)
    for g in range(bias_ref.shape[0]):
        for c in range(n_col):
            bias_ref[g, 0, c] = bias.astype(BF)


def bin_weights(w_bins, same_chain):
    n_feat = -(-(w_bins.shape[0] + 1) // 16) * 16
    rows = jnp.concatenate([w_bins, same_chain[None]], axis=0)
    rows = jnp.pad(rows, ((0, n_feat - rows.shape[0]), (0, 0)))
    high = lax.reduce_precision(rows, 8, 7)
    return jnp.concatenate([high, high, rows - high], axis=0).astype(BF)


def update(sizes, place, back, keep, other, near, far, gains, wgo, wout, wbins, wbias_t, n_heads, n_bins):
    ch, n_in, _ = back.shape
    n_col, sub, half, _ = keep.shape
    n_q = n_col * half
    n_rh, n_core, _ = sizes
    n_pa = n_core * sub
    n_row = sub
    n_in8 = -(-n_in // 8) * 8
    fixed = lambda i: (0, 0)
    row = lambda i: (i, 0, 0)
    return pl.pallas_call(
        functools.partial(update_kernel, n_bins),
        grid=(n_pa // n_row,),
        in_specs=[
            pl.BlockSpec(memory_space=pltpu.SMEM),
            pl.BlockSpec(back.shape, lambda i: (0, 0, 0)),
            pl.BlockSpec((n_col, n_row, half, ch), lambda i: (0, 0, 0, 0)),
            pl.BlockSpec((n_col, n_row, half, ch), lambda i: (0, 0, 0, 0)),
            pl.BlockSpec(memory_space=pltpu.SMEM),
            pl.BlockSpec(far.shape, fixed),
            pl.BlockSpec((1, ch), fixed),
            pl.BlockSpec((ch, 1), fixed),
            pl.BlockSpec((1, ch), fixed),
            pl.BlockSpec(wgo.shape, fixed),
            pl.BlockSpec(wout.shape, fixed),
            pl.BlockSpec(wbins.shape, fixed),
            pl.BlockSpec(wbias_t.shape, fixed),
        ],
        out_specs=[
            pl.BlockSpec((n_row, n_q, ch), row),
            pl.BlockSpec((n_row, n_q, ch), row),
            pl.BlockSpec(
                (n_rh, 1, n_col, sub * n_heads, n_q), lambda i: (0, i, 0, 0, 0)
            ),
        ],
        out_shape=[
            jax.ShapeDtypeStruct((n_pa, n_q, ch), BF),
            jax.ShapeDtypeStruct((n_pa, n_q, ch), BF),
            jax.ShapeDtypeStruct((n_rh, n_core, n_col, sub * n_heads, n_q), BF),
        ],
        scratch_shapes=[pltpu.VMEM((ch * n_in8, LANES), F32)],
        name="update",
    )(place, back, keep, other, near, far, gains[0], gains[1], gains[2], wgo, wout, wbins, wbias_t)


def project_kernel(
    core_ref, own_ref, other_ref, wq_ref, wk_ref, wv_ref, wg_ref, q_ref, k_ref, vt_ref, gate_ref
):
    n_heads, tall, n_k = vt_ref.shape[1:]
    head = wv_ref.shape[0] // n_heads
    first = core_ref[0] == 0
    n_row, n_q, ch = own_ref.shape
    own, other = own_ref[...], other_ref[...]
    full = jnp.concatenate(
        [jnp.where(first, own, other), jnp.where(first, other, own)], axis=1
    ).reshape(n_row * n_k, ch)
    own = own.reshape(n_row * n_q, ch)
    scale = LOG2E / math.sqrt(head)
    q_ref[...] = (dot(own, wq_ref[...]) * scale).astype(BF).reshape(n_row, n_q, ch)
    gate = jax.nn.sigmoid(dot_nt(wg_ref[...], own))
    k_ref[...] = dot(full, wk_ref[...]).astype(BF).reshape(n_row, n_k, ch)
    v_t = dot_nt(wv_ref[...], full).astype(BF)
    for r in range(n_row):
        gate_ref[r] = gate[:, r * n_q : (r + 1) * n_q]
        for h in range(n_heads):
            vt_ref[r, h, :head] = v_t[h * head : (h + 1) * head, r * n_k : (r + 1) * n_k]
            vt_ref[r, h, head:] = jnp.ones((tall - head, n_k), BF)


def project(core, own, other, wq, wk, wv_t, wg_t, n_heads, n_row=4):
    n_rows, n_q, ch = own.shape
    tall = ch // n_heads + 16
    row = lambda i: (i, 0, 0)
    fixed = pl.BlockSpec((ch, ch), lambda i: (0, 0))
    return pl.pallas_call(
        project_kernel,
        grid=(n_rows // n_row,),
        in_specs=[
            pl.BlockSpec(memory_space=pltpu.SMEM),
            pl.BlockSpec((n_row, n_q, ch), row),
            pl.BlockSpec((n_row, n_q, ch), row),
            fixed,
            fixed,
            fixed,
            fixed,
        ],
        out_specs=[
            pl.BlockSpec((n_row, n_q, ch), row),
            pl.BlockSpec((n_row, 2 * n_q, ch), row),
            pl.BlockSpec((n_row, n_heads, tall, 2 * n_q), lambda i: (i, 0, 0, 0)),
            pl.BlockSpec((n_row, ch, n_q), row),
        ],
        out_shape=[
            jax.ShapeDtypeStruct((n_rows, n_q, ch), BF),
            jax.ShapeDtypeStruct((n_rows, 2 * n_q, ch), BF),
            jax.ShapeDtypeStruct((n_rows, n_heads, tall, 2 * n_q), BF),
            jax.ShapeDtypeStruct((n_rows, ch, n_q), F32),
        ],
        name="project",
    )(core, own, other, wq, wk, wv_t, wg_t)


def attention_kernel(
    q_ref, k_ref, vt_ref, gate_ref, two_ref, bias_ref, wo_ref, out_ref, raw_sc, bias_sc
):
    n_unit, n_k, _ = bias_sc.shape
    n_q, ch = q_ref.shape[1:]
    n_heads, tall, _ = vt_ref.shape[1:]
    head = ch // n_heads
    n_src, n_pay, _ = bias_ref.shape
    n_lt = n_q // LANES
    n_rh = n_src // 16
    n_col, _, half, _ = out_ref.shape[1:]
    sub = n_q // n_rh // n_col
    pairs = n_heads // 2

    @pl.when(pl.program_id(0) == 0)
    def _():
        def widen(d, carry):
            for v in range(4):
                at = pl.multiple_of((d * 4 + v) * n_pay, 8)
                for t in range(n_lt):
                    part = bias_ref[d * 4 + v, :, t * LANES : (t + 1) * LANES]
                    raw_sc[t, pl.ds(at, n_pay), :] = part.astype(F32) * -LOG2E
            return carry

        lax.fori_loop(0, n_src // 4, widen, 0)

        def turn(i, carry):
            s, h = i // n_heads, i % n_heads
            for u in range(n_lt):
                for t in range(n_lt):
                    rows = []
                    for r in range(16 * t, 16 * (t + 1)):
                        at = (r // sub * 2 + s) * n_col * n_pay + r % sub * n_heads + h
                        rows.append(raw_sc[u, pl.ds(at, n_col, stride=n_pay), :])
                    block = jnp.concatenate(rows, axis=0).T
                    at_k = pl.multiple_of(s * n_q + u * LANES, LANES)
                    at_q = pl.multiple_of(h % 2 * LANES, LANES)
                    bias_sc[t * pairs + h // 2, pl.ds(at_k, LANES), pl.ds(at_q, LANES)] = block
            return carry

        lax.fori_loop(0, 2 * n_heads, turn, 0)

    def row(r, carry):
        k = k_ref[r]
        lane_head = lax.broadcasted_iota(jnp.int32, (LANES, ch), 1) // head
        zero = jnp.zeros((), BF)

        def scores(n):
            t, hp = divmod(n, pairs)
            rows = q_ref[r, t * LANES : (t + 1) * LANES, :]
            both = [jnp.where(lane_head == 2 * hp + v, rows, zero) for v in range(2)]
            return dot_nt(k, jnp.concatenate(both, axis=0))

        s = scores(0)
        parts = []
        for n in range(n_unit):
            t, hp = divmod(n, pairs)
            ahead = scores(n + 1) if n + 1 < n_unit else None
            s = s - bias_sc[n]
            p = jnp.exp2(s - jnp.max(s, axis=0, keepdims=True)).astype(BF)
            both = vt_ref[r, 2 * hp : 2 * hp + 2].reshape(2 * tall, n_k)
            o = dot(both, p)
            for v in range(2):
                block = o[v * tall : (v + 1) * tall, v * LANES : (v + 1) * LANES]
                parts.append(block[:head] / block[head : head + 1])
            if hp == pairs - 1:
                cols = slice(t * LANES, (t + 1) * LANES)
                gated = (gate_ref[r, :, cols] * jnp.concatenate(parts, axis=0)).astype(BF)
                parts = []
                res = lax.dot_general(
                    gated, wo_ref[...], (((0,), (0,)), ((), ())), preferred_element_type=F32
                )
                res = (two_ref[r, cols, :].astype(F32) + res).astype(BF)
                at = t * LANES
                while at < (t + 1) * LANES:
                    c, off = divmod(at, half)
                    size = min(half - off, (t + 1) * LANES - at)
                    out_ref[0, c, r, off : off + size] = res[at - t * LANES : at - t * LANES + size]
                    at += size
            s = ahead
        return carry

    lax.fori_loop(0, q_ref.shape[0], row, 0)


def attention(q, k, vt, gate, two, bias, wo, n_col, n_row=3):
    n_rows, n_q, ch = q.shape
    n_src, n_pay, _ = bias.shape
    n_heads = vt.shape[1]
    n_lt = n_q // LANES
    half = n_q // n_col
    steps = n_rows // 2 // n_row
    row = lambda i: (i, 0, 0)
    return pl.pallas_call(
        attention_kernel,
        grid=(2 * steps,),
        in_specs=[
            pl.BlockSpec((n_row, n_q, ch), row),
            pl.BlockSpec((n_row, 2 * n_q, ch), row),
            pl.BlockSpec((n_row,) + vt.shape[1:], lambda i: (i, 0, 0, 0)),
            pl.BlockSpec((n_row, ch, n_q), row),
            pl.BlockSpec((n_row, n_q, ch), row),
            pl.BlockSpec(bias.shape, lambda i: (0, 0, 0)),
            pl.BlockSpec(wo.shape, lambda i: (0, 0)),
        ],
        out_specs=pl.BlockSpec(
            (1, n_col, n_row, half, ch), lambda i: (i // steps, 0, i % steps, 0, 0)
        ),
        out_shape=jax.ShapeDtypeStruct((2, n_col, n_rows // 2, half, ch), BF),
        scratch_shapes=[
            pltpu.VMEM((n_lt, n_src * n_pay, LANES), F32),
            pltpu.VMEM((n_lt * n_heads // 2, 2 * n_q, 2 * LANES), F32),
        ],
        name="attention",
    )(q, k, vt, gate, two, bias, wo)


def body(
    pair_in,
    coords,
    chain_ids,
    coord_mask,
    gain_tri,
    gain_sum,
    gain_attn,
    w_tri_in,
    w_tri_out,
    w_bins,
    same_chain,
    w_query,
    w_attn,
    w_bias,
    w_attn_out,
):
    n_rh, n_core, n_col = (lax.axis_size(a) for a in ("rh", "core", "col"))
    rh, core, col = (lax.axis_index(a) for a in ("rh", "core", "col"))
    n_dev = n_rh * n_core * n_col
    every = ("rh", "core", "col")
    row_count, col_count, ch = pair_in.shape
    n_heads = w_bias.shape[1]
    n_bins = w_bins.shape[0]
    sub = row_count // n_col
    half = col_count // n_core
    n_pa = n_core * sub
    n_q = n_col * half

    packed = jnp.concatenate(
        [coords, chain_ids.astype(F32)[None], coord_mask.astype(F32)[None]], axis=0
    )
    packed = jnp.broadcast_to(packed, (n_rh * n_core, *packed.shape))
    known = exchange(packed, ("rh", "core"))
    known = known.reshape(n_rh, n_core, -1, row_count)

    w_sides = w_tri_in[:, : 4 * ch].T
    sides, *pieces = make_sides(col.reshape(1), pair_in, gain_tri, w_sides, n_col)
    sides = exchange(sides, every)

    pieces = [pieces[0]] + [
        lax.ppermute(pieces[d], "col", [(i, (i + d) % n_col) for i in range(n_col)])
        for d in range(1, n_col)
    ]
    whole = jnp.stack(pieces).reshape(n_col, sub, n_core, half, ch)
    keep = lax.dynamic_index_in_dim(whole, core, 2, keepdims=False)
    give = lax.dynamic_index_in_dim(whole, 1 - core, 2, keepdims=False)
    other_pair = lax.ppermute(give, "core", [(0, 1), (1, 0)])

    near = lax.dynamic_index_in_dim(known, rh, 0, keepdims=False)
    near = near.transpose(1, 0, 2).reshape(-1, n_core, sub, n_col)
    near = lax.dynamic_index_in_dim(near, col, 3, keepdims=False).reshape(-1, n_pa)
    far = lax.dynamic_index_in_dim(known, core, 1, keepdims=False)
    far = far.transpose(1, 0, 2).reshape(-1, n_q)

    product = triangle(sides, n_rh, n_core, n_col, row_count, col_count)
    back = exchange(product, every)
    two, normed, bias = update(
        (n_rh, n_core, n_col),
        jnp.stack([core, col]),
        back,
        keep,
        other_pair,
        near,
        far,
        (gain_tri.reshape(1, ch), gain_sum.reshape(ch, 1), gain_attn.reshape(1, ch)),
        w_tri_in[:, 4 * ch :],
        w_tri_out,
        bin_weights(w_bins, same_chain),
        jnp.pad(w_bias.T, ((0, 16 - n_heads), (0, 0))),
        n_heads,
        n_bins,
    )

    spread = exchange(bias.reshape(n_dev, sub * n_heads, n_q), every)
    other = lax.ppermute(normed, every, [(d, d ^ n_col) for d in range(n_dev)])
    q, k, v_t, gate = project(
        core.reshape(1),
        normed,
        other,
        w_query,
        w_attn[:, :ch],
        w_attn[:, ch : 2 * ch].T,
        w_attn[:, 2 * ch :].T,
        n_heads,
    )
    result = attention(q, k, v_t, gate, two, spread, w_attn_out, n_col)
    home = exchange(result.reshape(n_core * n_col, sub, half, ch), ("core", "col"))
    return (
        home.reshape(n_core, n_col, sub, half, ch)
        .transpose(2, 1, 0, 3, 4)
        .reshape(row_count, col_count, ch)
    )


def solution(mesh):
    n_row, n_col = mesh.shape["row"], mesh.shape["col"]
    split = Mesh(mesh.devices.reshape(n_row // 2, 2, n_col), ("rh", "core", "col"))
    row = ("rh", "core")

    return jax.shard_map(
        body,
        mesh=split,
        in_specs=(P(row, "col", None), P(None, row), P(row), P(row)) + (P(),) * 11,
        out_specs=P(row, "col", None),
        check_vma=False,
    )
```

```python
import functools
import math

import jax
import jax.numpy as jnp
from jax import lax
from jax.experimental import pallas as pl
from jax.experimental.pallas import tpu as pltpu
from jax.sharding import Mesh
from jax.sharding import PartitionSpec as P

BF = jnp.bfloat16
F32 = jnp.float32
LOG2E = 1.4426950408889634
NT = (((1,), (1,)), ((), ()))
LANES = 128


def layer_norm(values, gain):
    center = values - jnp.mean(values, axis=-1, keepdims=True)
    spread = jnp.mean(center * center, axis=-1, keepdims=True)
    return center * lax.rsqrt(spread + 1e-05) * gain


def dot(a, b):
    return jnp.dot(a, b, preferred_element_type=F32)


def dot_nt(a, b):
    return lax.dot_general(a, b, NT, preferred_element_type=F32)


def exchange(x, axes):
    return lax.all_to_all(x, axes, split_axis=0, concat_axis=0, tiled=True)


def sides_kernel(col_ref, x_ref, gain_ref, w_ref, out_ref, *rest_refs):
    piece_refs, norm_sc, sc = rest_refs[:-2], rest_refs[-2], rest_refs[-1]
    n_rows, n_cols, ch = x_ref.shape
    n_col = len(piece_refs)
    for shift, piece_ref in enumerate(piece_refs):
        for a in range(n_rows // n_col):
            piece_ref[a] = x_ref[a * n_col + (col_ref[0] + shift) % n_col]
    n_out = out_ref.shape[1]
    third = n_rows // 3
    cut = LANES - n_cols

    def norm(i, carry):
        for u in range(4):
            norm_sc[i * 4 + u] = layer_norm(x_ref[i * 4 + u].astype(F32), gain_ref[...]).astype(BF)
        return carry

    lax.fori_loop(0, n_rows // 4, norm, 0, unroll=2)

    def sides(x):
        pr = dot_nt(w_ref[...], x)
        left = jax.nn.sigmoid(pr[:ch]) * pr[ch : 2 * ch]
        right = jax.nn.sigmoid(pr[2 * ch : 3 * ch]) * pr[3 * ch :]
        return left, right

    def put(row, value):
        sc[pl.ds(row, ch, stride=n_out), :] = value

    def main(s, carry):
        x = jnp.concatenate(
            [
                norm_sc[s],
                norm_sc[third + s, :cut],
                norm_sc[2 * third + s],
                norm_sc[third + s, cut : 2 * cut],
            ],
            axis=0,
        )
        left, right = sides(x)
        put(s, left[:, :LANES])
        put(third + s, left[:, LANES:])
        put(2 * third + s, right[:, :LANES])
        put(3 * third + s, right[:, LANES:])
        return carry

    lax.fori_loop(0, third, main, 0, unroll=4)

    is_left = lax.broadcasted_iota(jnp.int32, (ch, LANES), 1) < LANES // 2

    def rest(s, carry):
        one = norm_sc[third + s, 2 * cut :]
        two = norm_sc[third + third // 2 + s, 2 * cut :]
        left, right = sides(jnp.concatenate([one, two, one, two], axis=0))
        put(4 * third + s, jnp.where(is_left, left, right))
        return carry

    lax.fori_loop(0, third // 2, rest, 0, unroll=4)

    def emit(c, carry):
        out_ref[c] = sc[pl.ds(pl.multiple_of(c * n_out, 8), n_out), :].astype(BF)
        return carry

    lax.fori_loop(0, ch, emit, 0, unroll=16)


def make_sides(col, pair, gain, w_t, n_col):
    n_rows, n_cols, ch = pair.shape
    n_out = 2 * n_rows * n_cols // LANES
    piece = jax.ShapeDtypeStruct((n_rows // n_col, n_cols, ch), BF)
    return pl.pallas_call(
        sides_kernel,
        in_specs=[pl.BlockSpec(memory_space=pltpu.SMEM)] + [pl.BlockSpec()] * 3,
        out_shape=[jax.ShapeDtypeStruct((ch, n_out, LANES), BF)] + [piece] * n_col,
        scratch_shapes=[
            pltpu.VMEM(pair.shape, BF),
            pltpu.VMEM((ch * n_out, LANES), F32),
        ],
        name="sides",
    )(col, pair, gain.reshape(1, ch), w_t)


def triangle_kernel(n_rh, n_core, n_col, n_rows, n_cols, in_ref, table_ref, out_ref, l_sc, r_sc, p_sc):
    third = n_rows // 3
    cut = LANES - n_cols
    total = n_rh * n_core * n_rows
    n_pa = n_core * n_rows // n_col
    n_lt = total // n_core // LANES
    lane = lax.broadcasted_iota(jnp.int32, (third, LANES), 1)

    def middle(a, b, c):
        return jnp.where(
            lane < cut,
            pltpu.roll(a, cut, 1),
            jnp.where(lane < 2 * cut, pltpu.roll(b, 2 * cut, 1), jnp.where(lane < n_cols, c, 0.0)),
        )

    def unpack(rh, carry):
        for p in range(n_core):
            for c in range(n_col):
                blk = in_ref[(rh * n_core + p) * n_col + c].astype(F32)
                b = [blk[third * t : third * (t + 1)] for t in range(4)]
                last = blk[4 * third :]
                keep = [jnp.where(lane < n_cols, t, 0.0) for t in b]
                lc = jnp.concatenate([pltpu.roll(last, 2 * cut, 1), pltpu.roll(last, cut, 1)], axis=0)
                rc = jnp.concatenate([last, pltpu.roll(last, 3 * cut, 1)], axis=0)
                left = jnp.concatenate([keep[0], middle(b[0], b[1], lc), keep[1]], axis=0)
                right = jnp.concatenate([keep[2], middle(b[2], b[3], rc), keep[3]], axis=0)
                lanes = slice(c * LANES, (c + 1) * LANES)
                at_l = pl.multiple_of((rh * n_core + p) * n_rows, 16)
                at_r = pl.multiple_of((p * n_rh + rh) * n_rows, 16)
                l_sc[pl.ds(at_l, n_rows), lanes] = left.astype(BF)
                r_sc[pl.ds(at_r, n_rows), lanes] = right.astype(BF)
        return carry

    lax.fori_loop(0, n_rh, unpack, 0)
    wide = 2 * LANES
    for t in range(total // wide):
        part = dot_nt(l_sc[...], r_sc[t * wide : (t + 1) * wide, :])
        p_sc[2 * t] = part[:, :LANES]
        p_sc[2 * t + 1] = part[:, LANES:]

    def pack(rh, carry):
        for core in range(n_core):
            for c in range(n_col):
                rows = pl.ds(rh * n_core * n_rows + c, n_pa, stride=n_col)
                parts = [p_sc[core * n_lt + t, rows, :] for t in range(n_lt)]
                out_ref[(rh * n_core + core) * n_col + c] = jnp.concatenate(parts, axis=0).astype(BF)
        return carry

    lax.fori_loop(0, n_rh, pack, 0)


def triangle(sides, table, n_rh, n_core, n_col, n_rows, n_cols):
    total = n_rh * n_core * n_rows
    n_pa = n_core * n_rows // n_col
    n_lt = total // n_core // LANES
    return pl.pallas_call(
        functools.partial(triangle_kernel, n_rh, n_core, n_col, n_rows, n_cols),
        in_specs=[pl.BlockSpec(), pl.BlockSpec(memory_space=pl.ANY)],
        out_shape=jax.ShapeDtypeStruct((sides.shape[0], n_lt * n_pa, LANES), BF),
        scratch_shapes=[
            pltpu.VMEM((total, n_col * LANES), BF),
            pltpu.VMEM((total, n_col * LANES), BF),
            pltpu.VMEM((total // LANES, total, LANES), F32),
        ],
        compiler_params=pltpu.CompilerParams(vmem_limit_bytes=24 << 20),
        name="triangle",
    )(sides, table)


def unit_norm(x, ones):
    center = x.astype(F32) - dot(x, ones[: x.shape[1]])
    square = center * center
    high = square.astype(BF)
    low = (square - high.astype(F32)).astype(BF)
    spread = dot(jnp.concatenate([high, low], axis=1), ones)
    return center * lax.rsqrt(spread + 1e-05)


def update_kernel(
    n_bins,
    place_ref,
    back_ref,
    keep_ref,
    other_ref,
    near_ref,
    far_ref,
    gain_tri_ref,
    gain_sum_ref,
    gain_attn_ref,
    wgo_ref,
    wout_ref,
    wbins_ref,
    wbias_ref,
    two_ref,
    normed_ref,
    bias_ref,
    sc,
):
    ch, n_in, _ = back_ref.shape
    n_q = far_ref.shape[1]
    n_lt = n_q // LANES
    n_pa = n_in // n_lt
    n_in8 = sc.shape[0] // ch
    n_col = keep_ref.shape[0]
    n_heads = bias_ref.shape[3] // two_ref.shape[0]
    tn = (((0,), (0,)), ((), ()))

    @pl.when(pl.program_id(0) == 0)
    def _():
        def widen(c, carry):
            sc[pl.ds(pl.multiple_of(c * n_in8, 8), n_in), :] = back_ref[c].astype(F32)
            return carry

        lax.fori_loop(0, ch, widen, 0, unroll=16)

    ones = jnp.full((2 * ch, ch), 1.0 / ch, BF)
    n_row = two_ref.shape[0]
    n_feat = wbins_ref.shape[0] // 3
    bin_at = lax.broadcasted_iota(jnp.int32, (n_feat, 1), 0)
    centres = 2.0 + 20.0 * bin_at.astype(F32) / (n_bins - 1)
    parts = []
    pairs = []
    feats = []
    for v in range(n_row):
        pa = pl.program_id(0) * n_row + v
        for t in range(n_lt):
            x = sc[pl.ds(t * n_pa + pa, ch, stride=n_in8), :]
            center = x - jnp.mean(x, axis=0, keepdims=True)
            spread = jnp.mean(center * center, axis=0, keepdims=True)
            parts.append((center * lax.rsqrt(spread + 1e-05) * gain_sum_ref[...]).astype(BF))
        mine = place_ref[0] == pl.program_id(0) * n_row // (n_pa // 2)
        for c in range(n_col):
            shift = (place_ref[1] + n_col - c) % n_col
            pairs.append(jnp.where(mine, keep_ref[shift, v], other_ref[shift, v]))
        square = jnp.zeros((1, n_q), F32)
        for f in range(3):
            off = far_ref[f : f + 1, :] - near_ref[f, pa]
            square = square + off * off
        shared = (far_ref[3:4, :] == near_ref[3, pa]).astype(F32)
        mask = far_ref[4:5, :] * near_ref[4, pa]
        z = (jnp.sqrt(square + 1.0) - centres) * ((n_bins - 1) / 25.0)
        bins = jnp.exp(-(z * z)) * mask
        feats.append(jnp.where(bin_at < n_bins, bins, jnp.where(bin_at == n_bins, shared, 0.0)))
    tri = lax.dot_general(
        jnp.concatenate(parts, axis=1), wout_ref[...], tn, preferred_element_type=F32
    )
    pair = jnp.concatenate(pairs, axis=0)
    normed_pair = (unit_norm(pair, ones) * gain_tri_ref[...]).astype(BF)
    gate = jax.nn.sigmoid(dot(normed_pair, wgo_ref[...]))
    feats = jnp.concatenate(feats, axis=1)
    high = feats.astype(BF)
    low = (feats - high.astype(F32)).astype(BF)
    binned = lax.dot_general(
        jnp.concatenate([high, low, high], axis=0), wbins_ref[...], tn, preferred_element_type=F32
    )
    two = (pair.astype(F32) + gate * tri + binned).astype(BF)
    normed = (unit_norm(two, ones) * gain_attn_ref[...]).astype(BF)
    bias = dot_nt(wbias_ref[...], normed)[:n_heads]
    for v in range(n_row):
        two_ref[v] = two[v * n_q : (v + 1) * n_q]
        normed_ref[v] = normed[v * n_q : (v + 1) * n_q]
    bias = jnp.concatenate([bias[:, v * n_q : (v + 1) * n_q] for v in range(n_row)], axis=0)
    for g in range(bias_ref.shape[0]):
        for c in range(n_col):
            bias_ref[g, 0, c] = bias.astype(BF)


def bin_weights(w_bins, same_chain):
    n_feat = -(-(w_bins.shape[0] + 1) // 16) * 16
    rows = jnp.concatenate([w_bins, same_chain[None]], axis=0)
    rows = jnp.pad(rows, ((0, n_feat - rows.shape[0]), (0, 0)))
    high = lax.reduce_precision(rows, 8, 7)
    return jnp.concatenate([high, high, rows - high], axis=0).astype(BF)


def update(sizes, place, back, keep, other, near, far, gains, wgo, wout, wbins, wbias_t, n_heads, n_bins):
    ch, n_in, _ = back.shape
    n_col, sub, half, _ = keep.shape
    n_q = n_col * half
    n_rh, n_core, _ = sizes
    n_pa = n_core * sub
    n_row = sub
    n_in8 = -(-n_in // 8) * 8
    fixed = lambda i: (0, 0)
    row = lambda i: (i, 0, 0)
    return pl.pallas_call(
        functools.partial(update_kernel, n_bins),
        grid=(n_pa // n_row,),
        in_specs=[
            pl.BlockSpec(memory_space=pltpu.SMEM),
            pl.BlockSpec(back.shape, lambda i: (0, 0, 0)),
            pl.BlockSpec((n_col, n_row, half, ch), lambda i: (0, 0, 0, 0)),
            pl.BlockSpec((n_col, n_row, half, ch), lambda i: (0, 0, 0, 0)),
            pl.BlockSpec(memory_space=pltpu.SMEM),
            pl.BlockSpec(far.shape, fixed),
            pl.BlockSpec((1, ch), fixed),
            pl.BlockSpec((ch, 1), fixed),
            pl.BlockSpec((1, ch), fixed),
            pl.BlockSpec(wgo.shape, fixed),
            pl.BlockSpec(wout.shape, fixed),
            pl.BlockSpec(wbins.shape, fixed),
            pl.BlockSpec(wbias_t.shape, fixed),
        ],
        out_specs=[
            pl.BlockSpec((n_row, n_q, ch), row),
            pl.BlockSpec((n_row, n_q, ch), row),
            pl.BlockSpec(
                (n_rh, 1, n_col, sub * n_heads, n_q), lambda i: (0, i, 0, 0, 0)
            ),
        ],
        out_shape=[
            jax.ShapeDtypeStruct((n_pa, n_q, ch), BF),
            jax.ShapeDtypeStruct((n_pa, n_q, ch), BF),
            jax.ShapeDtypeStruct((n_rh, n_core, n_col, sub * n_heads, n_q), BF),
        ],
        scratch_shapes=[pltpu.VMEM((ch * n_in8, LANES), F32)],
        name="update",
    )(place, back, keep, other, near, far, gains[0], gains[1], gains[2], wgo, wout, wbins, wbias_t)


def project_kernel(
    core_ref, own_ref, other_ref, wq_ref, wk_ref, wv_ref, wg_ref, q_ref, k_ref, vt_ref, gate_ref
):
    n_heads, tall, n_k = vt_ref.shape[1:]
    head = wv_ref.shape[0] // n_heads
    first = core_ref[0] == 0
    n_row, n_q, ch = own_ref.shape
    own, other = own_ref[...], other_ref[...]
    full = jnp.concatenate(
        [jnp.where(first, own, other), jnp.where(first, other, own)], axis=1
    ).reshape(n_row * n_k, ch)
    own = own.reshape(n_row * n_q, ch)
    scale = LOG2E / math.sqrt(head)
    q_ref[...] = (dot(own, wq_ref[...]) * scale).astype(BF).reshape(n_row, n_q, ch)
    gate = jax.nn.sigmoid(dot_nt(wg_ref[...], own))
    k_ref[...] = dot(full, wk_ref[...]).astype(BF).reshape(n_row, n_k, ch)
    v_t = dot_nt(wv_ref[...], full).astype(BF)
    for r in range(n_row):
        gate_ref[r] = gate[:, r * n_q : (r + 1) * n_q]
        for h in range(n_heads):
            vt_ref[r, h, :head] = v_t[h * head : (h + 1) * head, r * n_k : (r + 1) * n_k]
            vt_ref[r, h, head:] = jnp.ones((tall - head, n_k), BF)


def project(core, own, other, wq, wk, wv_t, wg_t, n_heads, n_row=4):
    n_rows, n_q, ch = own.shape
    tall = ch // n_heads + 16
    row = lambda i: (i, 0, 0)
    fixed = pl.BlockSpec((ch, ch), lambda i: (0, 0))
    return pl.pallas_call(
        project_kernel,
        grid=(n_rows // n_row,),
        in_specs=[
            pl.BlockSpec(memory_space=pltpu.SMEM),
            pl.BlockSpec((n_row, n_q, ch), row),
            pl.BlockSpec((n_row, n_q, ch), row),
            fixed,
            fixed,
            fixed,
            fixed,
        ],
        out_specs=[
            pl.BlockSpec((n_row, n_q, ch), row),
            pl.BlockSpec((n_row, 2 * n_q, ch), row),
            pl.BlockSpec((n_row, n_heads, tall, 2 * n_q), lambda i: (i, 0, 0, 0)),
            pl.BlockSpec((n_row, ch, n_q), row),
        ],
        out_shape=[
            jax.ShapeDtypeStruct((n_rows, n_q, ch), BF),
            jax.ShapeDtypeStruct((n_rows, 2 * n_q, ch), BF),
            jax.ShapeDtypeStruct((n_rows, n_heads, tall, 2 * n_q), BF),
            jax.ShapeDtypeStruct((n_rows, ch, n_q), F32),
        ],
        name="project",
    )(core, own, other, wq, wk, wv_t, wg_t)


def attention_kernel(
    q_ref, k_ref, vt_ref, gate_ref, two_ref, bias_ref, wo_ref, out_ref, raw_sc, bias_sc
):
    n_unit, n_k, _ = bias_sc.shape
    n_q, ch = q_ref.shape[1:]
    n_heads, tall, _ = vt_ref.shape[1:]
    head = ch // n_heads
    n_src, n_pay, _ = bias_ref.shape
    n_lt = n_q // LANES
    n_rh = n_src // 16
    n_col, _, half, _ = out_ref.shape[1:]
    sub = n_q // n_rh // n_col
    pairs = n_heads // 2

    @pl.when(pl.program_id(0) == 0)
    def _():
        def widen(d, carry):
            for v in range(4):
                at = pl.multiple_of((d * 4 + v) * n_pay, 8)
                for t in range(n_lt):
                    part = bias_ref[d * 4 + v, :, t * LANES : (t + 1) * LANES]
                    raw_sc[t, pl.ds(at, n_pay), :] = part.astype(F32) * -LOG2E
            return carry

        lax.fori_loop(0, n_src // 4, widen, 0)

        def turn(i, carry):
            s, h = i // n_heads, i % n_heads
            for u in range(n_lt):
                for t in range(n_lt):
                    rows = []
                    for r in range(16 * t, 16 * (t + 1)):
                        at = (r // sub * 2 + s) * n_col * n_pay + r % sub * n_heads + h
                        rows.append(raw_sc[u, pl.ds(at, n_col, stride=n_pay), :])
                    block = jnp.concatenate(rows, axis=0).T
                    at_k = pl.multiple_of(s * n_q + u * LANES, LANES)
                    at_q = pl.multiple_of(h % 2 * LANES, LANES)
                    bias_sc[t * pairs + h // 2, pl.ds(at_k, LANES), pl.ds(at_q, LANES)] = block
            return carry

        lax.fori_loop(0, 2 * n_heads, turn, 0)

    def row(r, carry):
        k = k_ref[r]
        lane_head = lax.broadcasted_iota(jnp.int32, (LANES, ch), 1) // head
        zero = jnp.zeros((), BF)

        def scores(n):
            t, hp = divmod(n, pairs)
            rows = q_ref[r, t * LANES : (t + 1) * LANES, :]
            both = [jnp.where(lane_head == 2 * hp + v, rows, zero) for v in range(2)]
            return dot_nt(k, jnp.concatenate(both, axis=0))

        s = scores(0)
        parts = []
        for n in range(n_unit):
            t, hp = divmod(n, pairs)
            ahead = scores(n + 1) if n + 1 < n_unit else None
            s = s - bias_sc[n]
            p = jnp.exp2(s - jnp.max(s, axis=0, keepdims=True)).astype(BF)
            both = vt_ref[r, 2 * hp : 2 * hp + 2].reshape(2 * tall, n_k)
            o = dot(both, p)
            for v in range(2):
                block = o[v * tall : (v + 1) * tall, v * LANES : (v + 1) * LANES]
                parts.append(block[:head] / block[head : head + 1])
            if hp == pairs - 1:
                cols = slice(t * LANES, (t + 1) * LANES)
                gated = (gate_ref[r, :, cols] * jnp.concatenate(parts, axis=0)).astype(BF)
                parts = []
                res = lax.dot_general(
                    gated, wo_ref[...], (((0,), (0,)), ((), ())), preferred_element_type=F32
                )
                res = (two_ref[r, cols, :].astype(F32) + res).astype(BF)
                at = t * LANES
                while at < (t + 1) * LANES:
                    c, off = divmod(at, half)
                    size = min(half - off, (t + 1) * LANES - at)
                    out_ref[0, c, r, off : off + size] = res[at - t * LANES : at - t * LANES + size]
                    at += size
            s = ahead
        return carry

    lax.fori_loop(0, q_ref.shape[0], row, 0)


def attention(q, k, vt, gate, two, bias, wo, n_col, n_row=3):
    n_rows, n_q, ch = q.shape
    n_src, n_pay, _ = bias.shape
    n_heads = vt.shape[1]
    n_lt = n_q // LANES
    half = n_q // n_col
    steps = n_rows // 2 // n_row
    row = lambda i: (i, 0, 0)
    return pl.pallas_call(
        attention_kernel,
        grid=(2 * steps,),
        in_specs=[
            pl.BlockSpec((n_row, n_q, ch), row),
            pl.BlockSpec((n_row, 2 * n_q, ch), row),
            pl.BlockSpec((n_row,) + vt.shape[1:], lambda i: (i, 0, 0, 0)),
            pl.BlockSpec((n_row, ch, n_q), row),
            pl.BlockSpec((n_row, n_q, ch), row),
            pl.BlockSpec(bias.shape, lambda i: (0, 0, 0)),
            pl.BlockSpec(wo.shape, lambda i: (0, 0)),
        ],
        out_specs=pl.BlockSpec(
            (1, n_col, n_row, half, ch), lambda i: (i // steps, 0, i % steps, 0, 0)
        ),
        out_shape=jax.ShapeDtypeStruct((2, n_col, n_rows // 2, half, ch), BF),
        scratch_shapes=[
            pltpu.VMEM((n_lt, n_src * n_pay, LANES), F32),
            pltpu.VMEM((n_lt * n_heads // 2, 2 * n_q, 2 * LANES), F32),
        ],
        name="attention",
    )(q, k, vt, gate, two, bias, wo)


def body(
    pair_in,
    coords,
    chain_ids,
    coord_mask,
    gain_tri,
    gain_sum,
    gain_attn,
    w_tri_in,
    w_tri_out,
    w_bins,
    same_chain,
    w_query,
    w_attn,
    w_bias,
    w_attn_out,
):
    n_rh, n_core, n_col = (lax.axis_size(a) for a in ("rh", "core", "col"))
    rh, core, col = (lax.axis_index(a) for a in ("rh", "core", "col"))
    n_dev = n_rh * n_core * n_col
    every = ("rh", "core", "col")
    row_count, col_count, ch = pair_in.shape
    n_heads = w_bias.shape[1]
    n_bins = w_bins.shape[0]
    sub = row_count // n_col
    half = col_count // n_core
    n_pa = n_core * sub
    n_q = n_col * half

    w_sides = w_tri_in[:, : 4 * ch].T
    sides, *pieces = make_sides(col.reshape(1), pair_in, gain_tri, w_sides, n_col)
    sides = exchange(sides, every)

    pieces = [pieces[0]] + [
        lax.ppermute(pieces[d], "col", [(i, (i + d) % n_col) for i in range(n_col)])
        for d in range(1, n_col)
    ]
    whole = jnp.stack(pieces).reshape(n_col, sub, n_core, half, ch)
    keep = lax.dynamic_index_in_dim(whole, core, 2, keepdims=False)
    give = lax.dynamic_index_in_dim(whole, 1 - core, 2, keepdims=False)
    other_pair = lax.ppermute(give, "core", [(0, 1), (1, 0)])

    table = jnp.concatenate(
        [coords, chain_ids.astype(F32)[None], coord_mask.astype(F32)[None]], axis=0
    ).reshape(1, -1)
    n_row = n_rh * n_core
    for step in (1, 4):
        swaps = [[(r, r ^ (step * d)) for r in range(n_row)] for d in range(1, 4)]
        table = jnp.concatenate(
            [table] + [lax.ppermute(table, ("rh", "core"), swap) for swap in swaps], axis=0
        )
    at = jnp.arange(n_row) ^ (rh * n_core + core)
    known = table[at].reshape(n_rh, n_core, -1, row_count)
    near = lax.dynamic_index_in_dim(known, rh, 0, keepdims=False)
    near = near.transpose(1, 0, 2).reshape(-1, n_core, sub, n_col)
    near = lax.dynamic_index_in_dim(near, col, 3, keepdims=False).reshape(-1, n_pa)
    far = lax.dynamic_index_in_dim(known, core, 1, keepdims=False)
    far = far.transpose(1, 0, 2).reshape(-1, n_q)

    product = triangle(sides, table, n_rh, n_core, n_col, row_count, col_count)
    back = exchange(product, every)
    two, normed, bias = update(
        (n_rh, n_core, n_col),
        jnp.stack([core, col]),
        back,
        keep,
        other_pair,
        near,
        far,
        (gain_tri.reshape(1, ch), gain_sum.reshape(ch, 1), gain_attn.reshape(1, ch)),
        w_tri_in[:, 4 * ch :],
        w_tri_out,
        bin_weights(w_bins, same_chain),
        jnp.pad(w_bias.T, ((0, 16 - n_heads), (0, 0))),
        n_heads,
        n_bins,
    )

    spread = exchange(bias.reshape(n_dev, sub * n_heads, n_q), every)
    other = lax.ppermute(normed, every, [(d, d ^ n_col) for d in range(n_dev)])
    q, k, v_t, gate = project(
        core.reshape(1),
        normed,
        other,
        w_query,
        w_attn[:, :ch],
        w_attn[:, ch : 2 * ch].T,
        w_attn[:, 2 * ch :].T,
        n_heads,
    )
    result = attention(q, k, v_t, gate, two, spread, w_attn_out, n_col)
    home = exchange(result.reshape(n_core * n_col, sub, half, ch), ("core", "col"))
    return (
        home.reshape(n_core, n_col, sub, half, ch)
        .transpose(2, 1, 0, 3, 4)
        .reshape(row_count, col_count, ch)
    )


def solution(mesh):
    n_row, n_col = mesh.shape["row"], mesh.shape["col"]
    split = Mesh(mesh.devices.reshape(n_row // 2, 2, n_col), ("rh", "core", "col"))
    row = ("rh", "core")

    return jax.shard_map(
        body,
        mesh=split,
        in_specs=(P(row, "col", None), P(None, row), P(row), P(row)) + (P(),) * 11,
        out_specs=P(row, "col", None),
        check_vma=False,
    )
```

```python
import functools
import math

import jax
import jax.numpy as jnp
from jax import lax
from jax.experimental import pallas as pl
from jax.experimental.pallas import tpu as pltpu
from jax.sharding import Mesh
from jax.sharding import PartitionSpec as P

BF = jnp.bfloat16
F32 = jnp.float32
LOG2E = 1.4426950408889634
NT = (((1,), (1,)), ((), ()))
LANES = 128


def layer_norm(values, gain):
    center = values - jnp.mean(values, axis=-1, keepdims=True)
    spread = jnp.mean(center * center, axis=-1, keepdims=True)
    return center * lax.rsqrt(spread + 1e-05) * gain


def dot(a, b):
    return jnp.dot(a, b, preferred_element_type=F32)


def dot_nt(a, b):
    return lax.dot_general(a, b, NT, preferred_element_type=F32)


def exchange(x, axes):
    return lax.all_to_all(x, axes, split_axis=0, concat_axis=0, tiled=True)


def sides_kernel(col_ref, x_ref, gain_ref, w_ref, out_ref, *rest_refs):
    piece_refs, (norm_sc, sc, w_sc) = rest_refs[:-3], rest_refs[-3:]
    n_rows, n_cols, ch = x_ref.shape
    n_col = len(piece_refs)
    w_sc[...] = w_ref[:, : 4 * ch].astype(F32).T.astype(BF)
    for shift, piece_ref in enumerate(piece_refs):
        for a in range(n_rows // n_col):
            piece_ref[a] = x_ref[a * n_col + (col_ref[0] + shift) % n_col]
    n_out = out_ref.shape[1]
    third = n_rows // 3
    cut = LANES - n_cols

    def norm(i, carry):
        for u in range(4):
            norm_sc[i * 4 + u] = layer_norm(x_ref[i * 4 + u].astype(F32), gain_ref[...]).astype(BF)
        return carry

    lax.fori_loop(0, n_rows // 4, norm, 0, unroll=2)

    def sides(x):
        pr = dot_nt(w_sc[...], x)
        left = jax.nn.sigmoid(pr[:ch]) * pr[ch : 2 * ch]
        right = jax.nn.sigmoid(pr[2 * ch : 3 * ch]) * pr[3 * ch :]
        return left, right

    def put(row, value):
        sc[pl.ds(row, ch, stride=n_out), :] = value

    def main(s, carry):
        x = jnp.concatenate(
            [
                norm_sc[s],
                norm_sc[third + s, :cut],
                norm_sc[2 * third + s],
                norm_sc[third + s, cut : 2 * cut],
            ],
            axis=0,
        )
        left, right = sides(x)
        put(s, left[:, :LANES])
        put(third + s, left[:, LANES:])
        put(2 * third + s, right[:, :LANES])
        put(3 * third + s, right[:, LANES:])
        return carry

    lax.fori_loop(0, third, main, 0, unroll=4)

    is_left = lax.broadcasted_iota(jnp.int32, (ch, LANES), 1) < LANES // 2

    def rest(s, carry):
        one = norm_sc[third + s, 2 * cut :]
        two = norm_sc[third + third // 2 + s, 2 * cut :]
        left, right = sides(jnp.concatenate([one, two, one, two], axis=0))
        put(4 * third + s, jnp.where(is_left, left, right))
        return carry

    lax.fori_loop(0, third // 2, rest, 0, unroll=4)

    def emit(c, carry):
        out_ref[c] = sc[pl.ds(pl.multiple_of(c * n_out, 8), n_out), :].astype(BF)
        return carry

    lax.fori_loop(0, ch, emit, 0, unroll=16)


def make_sides(col, pair, gain, w, n_col):
    n_rows, n_cols, ch = pair.shape
    n_out = 2 * n_rows * n_cols // LANES
    piece = jax.ShapeDtypeStruct((n_rows // n_col, n_cols, ch), BF)
    return pl.pallas_call(
        sides_kernel,
        in_specs=[pl.BlockSpec(memory_space=pltpu.SMEM)] + [pl.BlockSpec()] * 3,
        out_shape=[jax.ShapeDtypeStruct((ch, n_out, LANES), BF)] + [piece] * n_col,
        scratch_shapes=[
            pltpu.VMEM(pair.shape, BF),
            pltpu.VMEM((ch * n_out, LANES), F32),
            pltpu.VMEM((4 * ch, ch), BF),
        ],
        name="sides",
    )(col, pair, gain.reshape(1, ch), w)


def triangle_kernel(n_rh, n_core, n_col, n_rows, n_cols, in_ref, table_ref, out_ref, l_sc, r_sc, p_sc):
    third = n_rows // 3
    cut = LANES - n_cols
    total = n_rh * n_core * n_rows
    n_pa = n_core * n_rows // n_col
    n_lt = total // n_core // LANES
    lane = lax.broadcasted_iota(jnp.int32, (third, LANES), 1)

    def middle(a, b, c):
        return jnp.where(
            lane < cut,
            pltpu.roll(a, cut, 1),
            jnp.where(lane < 2 * cut, pltpu.roll(b, 2 * cut, 1), jnp.where(lane < n_cols, c, 0.0)),
        )

    def unpack(rh, carry):
        for p in range(n_core):
            for c in range(n_col):
                blk = in_ref[(rh * n_core + p) * n_col + c].astype(F32)
                b = [blk[third * t : third * (t + 1)] for t in range(4)]
                last = blk[4 * third :]
                keep = [jnp.where(lane < n_cols, t, 0.0) for t in b]
                lc = jnp.concatenate([pltpu.roll(last, 2 * cut, 1), pltpu.roll(last, cut, 1)], axis=0)
                rc = jnp.concatenate([last, pltpu.roll(last, 3 * cut, 1)], axis=0)
                left = jnp.concatenate([keep[0], middle(b[0], b[1], lc), keep[1]], axis=0)
                right = jnp.concatenate([keep[2], middle(b[2], b[3], rc), keep[3]], axis=0)
                lanes = slice(c * LANES, (c + 1) * LANES)
                at_l = pl.multiple_of((rh * n_core + p) * n_rows, 16)
                at_r = pl.multiple_of((p * n_rh + rh) * n_rows, 16)
                l_sc[pl.ds(at_l, n_rows), lanes] = left.astype(BF)
                r_sc[pl.ds(at_r, n_rows), lanes] = right.astype(BF)
        return carry

    lax.fori_loop(0, n_rh, unpack, 0)
    wide = 2 * LANES
    for t in range(total // wide):
        part = dot_nt(l_sc[...], r_sc[t * wide : (t + 1) * wide, :])
        p_sc[2 * t] = part[:, :LANES]
        p_sc[2 * t + 1] = part[:, LANES:]

    def pack(rh, carry):
        for core in range(n_core):
            for c in range(n_col):
                rows = pl.ds(rh * n_core * n_rows + c, n_pa, stride=n_col)
                parts = [p_sc[core * n_lt + t, rows, :] for t in range(n_lt)]
                out_ref[(rh * n_core + core) * n_col + c] = jnp.concatenate(parts, axis=0).astype(BF)
        return carry

    lax.fori_loop(0, n_rh, pack, 0)


def triangle(sides, table, n_rh, n_core, n_col, n_rows, n_cols):
    total = n_rh * n_core * n_rows
    n_pa = n_core * n_rows // n_col
    n_lt = total // n_core // LANES
    return pl.pallas_call(
        functools.partial(triangle_kernel, n_rh, n_core, n_col, n_rows, n_cols),
        in_specs=[pl.BlockSpec(), pl.BlockSpec(memory_space=pl.ANY)],
        out_shape=jax.ShapeDtypeStruct((sides.shape[0], n_lt * n_pa, LANES), BF),
        scratch_shapes=[
            pltpu.VMEM((total, n_col * LANES), BF),
            pltpu.VMEM((total, n_col * LANES), BF),
            pltpu.VMEM((total // LANES, total, LANES), F32),
        ],
        compiler_params=pltpu.CompilerParams(vmem_limit_bytes=24 << 20),
        name="triangle",
    )(sides, table)


def split_kernel(core_ref, *refs):
    pieces, (keep_ref, give_ref) = refs[:-3], refs[-2:]
    half = keep_ref.shape[2]
    core = core_ref[0]
    for s, piece in enumerate(pieces):
        keep_ref[s] = piece[:, pl.ds(pl.multiple_of(core * half, 16), half), :]
        give_ref[s] = piece[:, pl.ds(pl.multiple_of((1 - core) * half, 16), half), :]


def split(core, pieces, product):
    sub, n_cols, ch = pieces[0].shape
    out = jax.ShapeDtypeStruct((len(pieces), sub, n_cols // 2, ch), BF)
    return pl.pallas_call(
        split_kernel,
        in_specs=[pl.BlockSpec(memory_space=pltpu.SMEM)]
        + [pl.BlockSpec()] * len(pieces)
        + [pl.BlockSpec(memory_space=pl.ANY)],
        out_shape=[out, out],
        name="split",
    )(core, *pieces, product)


def unit_norm(x, ones):
    center = x.astype(F32) - dot(x, ones[: x.shape[1]])
    square = center * center
    high = square.astype(BF)
    low = (square - high.astype(F32)).astype(BF)
    spread = dot(jnp.concatenate([high, low], axis=1), ones)
    return center * lax.rsqrt(spread + 1e-05)


def update_kernel(
    n_bins,
    place_ref,
    back_ref,
    keep_ref,
    other_ref,
    near_ref,
    far_ref,
    gain_tri_ref,
    gain_sum_ref,
    gain_attn_ref,
    wgo_ref,
    wout_ref,
    wbins_ref,
    wbias_ref,
    two_ref,
    normed_ref,
    bias_ref,
    sc,
):
    ch, n_in, _ = back_ref.shape
    n_q = far_ref.shape[1]
    n_lt = n_q // LANES
    n_pa = n_in // n_lt
    n_in8 = sc.shape[0] // ch
    n_col = keep_ref.shape[0]
    n_heads = bias_ref.shape[3] // two_ref.shape[0]
    tn = (((0,), (0,)), ((), ()))

    @pl.when(pl.program_id(0) == 0)
    def _():
        def widen(c, carry):
            sc[pl.ds(pl.multiple_of(c * n_in8, 8), n_in), :] = back_ref[c].astype(F32)
            return carry

        lax.fori_loop(0, ch, widen, 0, unroll=16)

    ones = jnp.full((2 * ch, ch), 1.0 / ch, BF)
    n_row = two_ref.shape[0]
    n_feat = wbins_ref.shape[0] // 3
    bin_at = lax.broadcasted_iota(jnp.int32, (n_feat, 1), 0)
    centres = 2.0 + 20.0 * bin_at.astype(F32) / (n_bins - 1)
    parts = []
    pairs = []
    feats = []
    for v in range(n_row):
        pa = pl.program_id(0) * n_row + v
        for t in range(n_lt):
            x = sc[pl.ds(t * n_pa + pa, ch, stride=n_in8), :]
            center = x - jnp.mean(x, axis=0, keepdims=True)
            spread = jnp.mean(center * center, axis=0, keepdims=True)
            parts.append((center * lax.rsqrt(spread + 1e-05) * gain_sum_ref[...]).astype(BF))
        mine = place_ref[0] == pl.program_id(0) * n_row // (n_pa // 2)
        for c in range(n_col):
            shift = (place_ref[1] + n_col - c) % n_col
            pairs.append(jnp.where(mine, keep_ref[shift, v], other_ref[shift, v]))
        square = jnp.zeros((1, n_q), F32)
        for f in range(3):
            off = far_ref[f : f + 1, :] - near_ref[f, pa]
            square = square + off * off
        shared = (far_ref[3:4, :] == near_ref[3, pa]).astype(F32)
        mask = far_ref[4:5, :] * near_ref[4, pa]
        z = (jnp.sqrt(square + 1.0) - centres) * ((n_bins - 1) / 25.0)
        bins = jnp.exp(-(z * z)) * mask
        feats.append(jnp.where(bin_at < n_bins, bins, jnp.where(bin_at == n_bins, shared, 0.0)))
    tri = lax.dot_general(
        jnp.concatenate(parts, axis=1), wout_ref[...], tn, preferred_element_type=F32
    )
    pair = jnp.concatenate(pairs, axis=0)
    normed_pair = (unit_norm(pair, ones) * gain_tri_ref[...]).astype(BF)
    gate = jax.nn.sigmoid(dot(normed_pair, wgo_ref[...]))
    feats = jnp.concatenate(feats, axis=1)
    high = feats.astype(BF)
    low = (feats - high.astype(F32)).astype(BF)
    binned = lax.dot_general(
        jnp.concatenate([high, low, high], axis=0), wbins_ref[...], tn, preferred_element_type=F32
    )
    two = (pair.astype(F32) + gate * tri + binned).astype(BF)
    normed = (unit_norm(two, ones) * gain_attn_ref[...]).astype(BF)
    bias = dot_nt(wbias_ref[...], normed)[:n_heads]
    for v in range(n_row):
        two_ref[v] = two[v * n_q : (v + 1) * n_q]
        normed_ref[v] = normed[v * n_q : (v + 1) * n_q]
    bias = jnp.concatenate([bias[:, v * n_q : (v + 1) * n_q] for v in range(n_row)], axis=0)
    for g in range(bias_ref.shape[0]):
        for c in range(n_col):
            bias_ref[g, 0, c] = bias.astype(BF)


def bin_weights(w_bins, same_chain):
    n_feat = -(-(w_bins.shape[0] + 1) // 16) * 16
    rows = jnp.concatenate([w_bins, same_chain[None]], axis=0)
    rows = jnp.pad(rows, ((0, n_feat - rows.shape[0]), (0, 0)))
    high = lax.reduce_precision(rows, 8, 7)
    return jnp.concatenate([high, high, rows - high], axis=0).astype(BF)


def update(sizes, place, back, keep, other, near, far, gains, wgo, wout, wbins, wbias_t, n_heads, n_bins):
    ch, n_in, _ = back.shape
    n_col, sub, half, _ = keep.shape
    n_q = n_col * half
    n_rh, n_core, _ = sizes
    n_pa = n_core * sub
    n_row = sub
    n_in8 = -(-n_in // 8) * 8
    fixed = lambda i: (0, 0)
    row = lambda i: (i, 0, 0)
    return pl.pallas_call(
        functools.partial(update_kernel, n_bins),
        grid=(n_pa // n_row,),
        in_specs=[
            pl.BlockSpec(memory_space=pltpu.SMEM),
            pl.BlockSpec(back.shape, lambda i: (0, 0, 0)),
            pl.BlockSpec((n_col, n_row, half, ch), lambda i: (0, 0, 0, 0)),
            pl.BlockSpec((n_col, n_row, half, ch), lambda i: (0, 0, 0, 0)),
            pl.BlockSpec(memory_space=pltpu.SMEM),
            pl.BlockSpec(far.shape, fixed),
            pl.BlockSpec((1, ch), fixed),
            pl.BlockSpec((ch, 1), fixed),
            pl.BlockSpec((1, ch), fixed),
            pl.BlockSpec(wgo.shape, fixed),
            pl.BlockSpec(wout.shape, fixed),
            pl.BlockSpec(wbins.shape, fixed),
            pl.BlockSpec(wbias_t.shape, fixed),
        ],
        out_specs=[
            pl.BlockSpec((n_row, n_q, ch), row),
            pl.BlockSpec((n_row, n_q, ch), row),
            pl.BlockSpec(
                (n_rh, 1, n_col, sub * n_heads, n_q), lambda i: (0, i, 0, 0, 0)
            ),
        ],
        out_shape=[
            jax.ShapeDtypeStruct((n_pa, n_q, ch), BF),
            jax.ShapeDtypeStruct((n_pa, n_q, ch), BF),
            jax.ShapeDtypeStruct((n_rh, n_core, n_col, sub * n_heads, n_q), BF),
        ],
        scratch_shapes=[pltpu.VMEM((ch * n_in8, LANES), F32)],
        compiler_params=pltpu.CompilerParams(vmem_limit_bytes=44 << 20),
        name="update",
    )(place, back, keep, other, near, far, gains[0], gains[1], gains[2], wgo, wout, wbins, wbias_t)


def project_kernel(
    core_ref, own_ref, other_ref, wq_ref, wk_ref, wv_ref, wg_ref, q_ref, k_ref, vt_ref, gate_ref
):
    n_heads, tall, n_k = vt_ref.shape[1:]
    head = wv_ref.shape[0] // n_heads
    first = core_ref[0] == 0
    n_row, n_q, ch = own_ref.shape
    own, other = own_ref[...], other_ref[...]
    full = jnp.concatenate(
        [jnp.where(first, own, other), jnp.where(first, other, own)], axis=1
    ).reshape(n_row * n_k, ch)
    own = own.reshape(n_row * n_q, ch)
    scale = LOG2E / math.sqrt(head)
    q_ref[...] = (dot(own, wq_ref[...]) * scale).astype(BF).reshape(n_row, n_q, ch)
    gate = jax.nn.sigmoid(dot_nt(wg_ref[...], own))
    k_ref[...] = dot(full, wk_ref[...]).astype(BF).reshape(n_row, n_k, ch)
    v_t = dot_nt(wv_ref[...], full).astype(BF)
    for r in range(n_row):
        gate_ref[r] = gate[:, r * n_q : (r + 1) * n_q]
        for h in range(n_heads):
            vt_ref[r, h, :head] = v_t[h * head : (h + 1) * head, r * n_k : (r + 1) * n_k]
            vt_ref[r, h, head:] = jnp.ones((tall - head, n_k), BF)


def project(core, own, other, wq, wk, wv_t, wg_t, n_heads, n_row=4):
    n_rows, n_q, ch = own.shape
    tall = ch // n_heads + 16
    row = lambda i: (i, 0, 0)
    fixed = pl.BlockSpec((ch, ch), lambda i: (0, 0))
    return pl.pallas_call(
        project_kernel,
        grid=(n_rows // n_row,),
        in_specs=[
            pl.BlockSpec(memory_space=pltpu.SMEM),
            pl.BlockSpec((n_row, n_q, ch), row),
            pl.BlockSpec((n_row, n_q, ch), row),
            fixed,
            fixed,
            fixed,
            fixed,
        ],
        out_specs=[
            pl.BlockSpec((n_row, n_q, ch), row),
            pl.BlockSpec((n_row, 2 * n_q, ch), row),
            pl.BlockSpec((n_row, n_heads, tall, 2 * n_q), lambda i: (i, 0, 0, 0)),
            pl.BlockSpec((n_row, ch, n_q), row),
        ],
        out_shape=[
            jax.ShapeDtypeStruct((n_rows, n_q, ch), BF),
            jax.ShapeDtypeStruct((n_rows, 2 * n_q, ch), BF),
            jax.ShapeDtypeStruct((n_rows, n_heads, tall, 2 * n_q), BF),
            jax.ShapeDtypeStruct((n_rows, ch, n_q), F32),
        ],
        name="project",
    )(core, own, other, wq, wk, wv_t, wg_t)


def attention_kernel(
    q_ref, k_ref, vt_ref, gate_ref, two_ref, bias_ref, wo_ref, out_ref, raw_sc, bias_sc
):
    n_unit, n_k, _ = bias_sc.shape
    n_q, ch = q_ref.shape[1:]
    n_heads, tall, _ = vt_ref.shape[1:]
    head = ch // n_heads
    n_src, n_pay, _ = bias_ref.shape
    n_lt = n_q // LANES
    n_rh = n_src // 16
    n_col, _, half, _ = out_ref.shape[1:]
    sub = n_q // n_rh // n_col
    pairs = n_heads // 2

    @pl.when(pl.program_id(0) == 0)
    def _():
        def widen(d, carry):
            for v in range(4):
                at = pl.multiple_of((d * 4 + v) * n_pay, 8)
                for t in range(n_lt):
                    part = bias_ref[d * 4 + v, :, t * LANES : (t + 1) * LANES]
                    raw_sc[t, pl.ds(at, n_pay), :] = part.astype(F32) * -LOG2E
            return carry

        lax.fori_loop(0, n_src // 4, widen, 0)

        def turn(i, carry):
            s, h = i // n_heads, i % n_heads
            for u in range(n_lt):
                for t in range(n_lt):
                    rows = []
                    for r in range(16 * t, 16 * (t + 1)):
                        at = (r // sub * 2 + s) * n_col * n_pay + r % sub * n_heads + h
                        rows.append(raw_sc[u, pl.ds(at, n_col, stride=n_pay), :])
                    block = jnp.concatenate(rows, axis=0).T
                    at_k = pl.multiple_of(s * n_q + u * LANES, LANES)
                    at_q = pl.multiple_of(h % 2 * LANES, LANES)
                    bias_sc[t * pairs + h // 2, pl.ds(at_k, LANES), pl.ds(at_q, LANES)] = block
            return carry

        lax.fori_loop(0, 2 * n_heads, turn, 0)

    def row(r, carry):
        k = k_ref[r]
        lane_head = lax.broadcasted_iota(jnp.int32, (LANES, ch), 1) // head
        zero = jnp.zeros((), BF)

        def scores(n):
            t, hp = divmod(n, pairs)
            rows = q_ref[r, t * LANES : (t + 1) * LANES, :]
            both = [jnp.where(lane_head == 2 * hp + v, rows, zero) for v in range(2)]
            return dot_nt(k, jnp.concatenate(both, axis=0))

        s = scores(0)
        parts = []
        for n in range(n_unit):
            t, hp = divmod(n, pairs)
            ahead = scores(n + 1) if n + 1 < n_unit else None
            s = s - bias_sc[n]
            p = jnp.exp2(s - jnp.max(s, axis=0, keepdims=True)).astype(BF)
            both = vt_ref[r, 2 * hp : 2 * hp + 2].reshape(2 * tall, n_k)
            o = dot(both, p)
            for v in range(2):
                block = o[v * tall : (v + 1) * tall, v * LANES : (v + 1) * LANES]
                parts.append(block[:head] / block[head : head + 1])
            if hp == pairs - 1:
                cols = slice(t * LANES, (t + 1) * LANES)
                gated = (gate_ref[r, :, cols] * jnp.concatenate(parts, axis=0)).astype(BF)
                parts = []
                res = lax.dot_general(
                    gated, wo_ref[...], (((0,), (0,)), ((), ())), preferred_element_type=F32
                )
                res = (two_ref[r, cols, :].astype(F32) + res).astype(BF)
                at = t * LANES
                while at < (t + 1) * LANES:
                    c, off = divmod(at, half)
                    size = min(half - off, (t + 1) * LANES - at)
                    out_ref[0, c, r, off : off + size] = res[at - t * LANES : at - t * LANES + size]
                    at += size
            s = ahead
        return carry

    lax.fori_loop(0, q_ref.shape[0], row, 0, unroll=3)


def attention(q, k, vt, gate, two, bias, wo, n_col, n_row=3):
    n_rows, n_q, ch = q.shape
    n_src, n_pay, _ = bias.shape
    n_heads = vt.shape[1]
    n_lt = n_q // LANES
    half = n_q // n_col
    steps = n_rows // 2 // n_row
    row = lambda i: (i, 0, 0)
    return pl.pallas_call(
        attention_kernel,
        grid=(2 * steps,),
        in_specs=[
            pl.BlockSpec((n_row, n_q, ch), row),
            pl.BlockSpec((n_row, 2 * n_q, ch), row),
            pl.BlockSpec((n_row,) + vt.shape[1:], lambda i: (i, 0, 0, 0)),
            pl.BlockSpec((n_row, ch, n_q), row),
            pl.BlockSpec((n_row, n_q, ch), row),
            pl.BlockSpec(bias.shape, lambda i: (0, 0, 0)),
            pl.BlockSpec(wo.shape, lambda i: (0, 0)),
        ],
        out_specs=pl.BlockSpec(
            (1, n_col, n_row, half, ch), lambda i: (i // steps, 0, i % steps, 0, 0)
        ),
        out_shape=jax.ShapeDtypeStruct((2, n_col, n_rows // 2, half, ch), BF),
        scratch_shapes=[
            pltpu.VMEM((n_lt, n_src * n_pay, LANES), F32),
            pltpu.VMEM((n_lt * n_heads // 2, 2 * n_q, 2 * LANES), F32),
        ],
        name="attention",
    )(q, k, vt, gate, two, bias, wo)


def body(
    pair_in,
    coords,
    chain_ids,
    coord_mask,
    gain_tri,
    gain_sum,
    gain_attn,
    w_tri_in,
    w_tri_out,
    w_bins,
    same_chain,
    w_query,
    w_attn,
    w_bias,
    w_attn_out,
):
    n_rh, n_core, n_col = (lax.axis_size(a) for a in ("rh", "core", "col"))
    rh, core, col = (lax.axis_index(a) for a in ("rh", "core", "col"))
    n_dev = n_rh * n_core * n_col
    every = ("rh", "core", "col")
    row_count, col_count, ch = pair_in.shape
    n_heads = w_bias.shape[1]
    n_bins = w_bins.shape[0]
    sub = row_count // n_col
    half = col_count // n_core
    n_pa = n_core * sub
    n_q = n_col * half

    sides, *pieces = make_sides(col.reshape(1), pair_in, gain_tri, w_tri_in, n_col)
    sides = exchange(sides, every)

    pieces = [pieces[0]] + [
        lax.ppermute(pieces[d], "col", [(i, (i + d) % n_col) for i in range(n_col)])
        for d in range(1, n_col)
    ]
    table = jnp.concatenate(
        [coords, chain_ids.astype(F32)[None], coord_mask.astype(F32)[None]], axis=0
    ).reshape(1, -1)
    n_row = n_rh * n_core
    for step in (1, 4):
        swaps = [[(r, r ^ (step * d)) for r in range(n_row)] for d in range(1, 4)]
        table = jnp.concatenate(
            [table] + [lax.ppermute(table, ("rh", "core"), swap) for swap in swaps], axis=0
        )
    at = jnp.arange(n_row) ^ (rh * n_core + core)
    known = table[at].reshape(n_rh, n_core, -1, row_count)
    near = lax.dynamic_index_in_dim(known, rh, 0, keepdims=False)
    near = near.transpose(1, 0, 2).reshape(-1, n_core, sub, n_col)
    near = lax.dynamic_index_in_dim(near, col, 3, keepdims=False).reshape(-1, n_pa)
    far = lax.dynamic_index_in_dim(known, core, 1, keepdims=False)
    far = far.transpose(1, 0, 2).reshape(-1, n_q)

    product = triangle(sides, table, n_rh, n_core, n_col, row_count, col_count)
    keep, give = split(core.reshape(1), pieces, product)
    other_pair = lax.ppermute(give, "core", [(0, 1), (1, 0)])
    back = exchange(product, every)
    two, normed, bias = update(
        (n_rh, n_core, n_col),
        jnp.stack([core, col]),
        back,
        keep,
        other_pair,
        near,
        far,
        (gain_tri.reshape(1, ch), gain_sum.reshape(ch, 1), gain_attn.reshape(1, ch)),
        w_tri_in[:, 4 * ch :],
        w_tri_out,
        bin_weights(w_bins, same_chain),
        jnp.pad(w_bias.T, ((0, 16 - n_heads), (0, 0))),
        n_heads,
        n_bins,
    )

    spread = exchange(bias.reshape(n_dev, sub * n_heads, n_q), every)
    other = lax.ppermute(normed, every, [(d, d ^ n_col) for d in range(n_dev)])
    q, k, v_t, gate = project(
        core.reshape(1),
        normed,
        other,
        w_query,
        w_attn[:, :ch],
        w_attn[:, ch : 2 * ch].T,
        w_attn[:, 2 * ch :].T,
        n_heads,
    )
    result = attention(q, k, v_t, gate, two, spread, w_attn_out, n_col)
    home = exchange(result.reshape(n_core * n_col, sub, half, ch), ("core", "col"))
    return (
        home.reshape(n_core, n_col, sub, half, ch)
        .transpose(2, 1, 0, 3, 4)
        .reshape(row_count, col_count, ch)
    )


def solution(mesh):
    n_row, n_col = mesh.shape["row"], mesh.shape["col"]
    split = Mesh(mesh.devices.reshape(n_row // 2, 2, n_col), ("rh", "core", "col"))
    row = ("rh", "core")

    return jax.shard_map(
        body,
        mesh=split,
        in_specs=(P(row, "col", None), P(None, row), P(row), P(row)) + (P(),) * 11,
        out_specs=P(row, "col", None),
        check_vma=False,
    )
```
